128 devices in a mesh: nodes: 2 (over core), gx: 8 (over y_lo, z), gy: 8 (over y_hi, x).
Axes of the slice: x: 4, y: 4 (y_hi: 2, y_lo: 2; y = y_hi * 2 + y_lo), z: 4, core: 2. Of those that a mesh axis runs over, the one named last changes fastest.
Arguments:
- field_modes: float32 [4, 9, 512, 1024], P(None, None, 'gx', 'gy'), may hold values from -4 to 4, as said below
- node_points: float32 [768, 8], replicated, may hold values from -1 to 1
- quad_weight: float32 [768], replicated, may hold values from 0.5 to 2
- group_of: int32 [768], replicated, may hold values from 0 to 2, as said below
Outputs:
- mean_field: float32 [512, 1024], P('gx', 'gy')
- variance_field: float32 [512, 1024], P('gx', 'gy')
The draws below stay inside these ranges and needn't reach their ends.
Inputs may be any that keep to these rules, and one draw needn't show every extreme that they name: `group_of`: one of the two groups (which one varies) is given exactly 384 nodes, the other between 48 and 96; all other nodes hold 2. `field_modes`: diffusivity fields (index 3) give a diffusivity between 0.1 and 1.4 at every node point in range; the other fields lie within the range.
All inputs are finite; a program needn't handle non-finite values.
Results may differ from the reference program's by a relative error of at most 0.00021.
Values sent between devices are 32-bit elements; how exact they have to be, the bound alone decides.
A program may use at most 192 MiB of HBM per device.

```python
import math
import jax
import jax.numpy as jnp
from jax import lax

BUSY = 384
STEPS = 4
DIMS = 8
NODES = 768
NX = 512
NY = 1024


def draw_group_of(key, part):
    key_busy = jax.random.fold_in(key, 11)
    key_light = jax.random.fold_in(key, 12)
    key_order = jax.random.fold_in(key, 13)
    busy_group = jax.random.randint(key_busy, (), 0, 2)
    light_count = jax.random.randint(key_light, (), BUSY // 8, BUSY // 4 + 1)
    ordering = jax.random.permutation(key_order, NODES)
    placed = jnp.argsort(ordering)
    labels = jnp.where(placed < BUSY, busy_group, jnp.where(placed < BUSY + light_count, 1 - busy_group, 2))
    return labels.astype(jnp.int32)


def draw_field_modes(key, part):
    keys = [jax.random.fold_in(key, 21 + number) for number in range(5)]
    shaped = (DIMS + 1, NX, NY)
    initial = jnp.clip(jax.random.normal(keys[0], shaped), -4.0, 4.0)
    speeds = jnp.clip(0.25 * jax.random.normal(keys[1], (2,) + shaped), -1.0, 1.0)
    diff_base = jax.random.uniform(keys[2], (1, NX, NY), minval=0.5, maxval=1.0)
    diff_modes = jax.random.uniform(keys[4], (DIMS, NX, NY), minval=-0.05, maxval=0.05)
    diffusion = jnp.concatenate([diff_base, diff_modes], axis=0)
    return jnp.stack([initial, speeds[0], speeds[1], diffusion]).astype(jnp.float32)


def setup_inputs(seed: int = 0) -> dict:
    splits = jax.random.split(jax.random.key(seed), 5)
    return {
        "field_modes": draw_field_modes(jax.random.fold_in(splits[4], 71), 0),
        "node_points": jnp.clip(jax.random.uniform(splits[1], (NODES, DIMS), jnp.float32, -1.0, 1.0), -1.0, 1.0),
        "quad_weight": jnp.clip(jnp.exp(jax.random.uniform(splits[2], (NODES,), jnp.float32, math.log(0.5), math.log(2.0))), 0.5, 2.0),
        "group_of": draw_group_of(jax.random.fold_in(splits[4], 71), 0),
    }


TIME_STEP = 0.15


def advance_cells(centre, east_side, west_side, north_side, south_side, x_speed, y_speed, diffusion):
    laplace = (east_side + west_side + north_side + south_side) - 4.0 * centre
    transport = x_speed * ((east_side - west_side) * 0.5) + y_speed * ((north_side - south_side) * 0.5)
    return centre + TIME_STEP * (diffusion * laplace - transport)


def evolve(coefficients, field_modes):
    params = jnp.einsum("bk,ckxy->bcxy", coefficients, field_modes, precision=lax.Precision.HIGHEST)
    state = params[:, 0]
    for section in range(STEPS):
        east_side = jnp.roll(state, -1, axis=1)
        west_side = jnp.roll(state, 1, axis=1)
        north_side = jnp.roll(state, -1, axis=2)
        south_side = jnp.roll(state, 1, axis=2)
        state = advance_cells(state, east_side, west_side, north_side, south_side, params[:, 1], params[:, 2], params[:, 3])
    return state


def reference(field_modes, node_points, quad_weight, group_of):
    included = (group_of < 2).astype(jnp.float32)
    weight = quad_weight * included
    weight_total = jnp.sum(weight)
    coefficients = jnp.concatenate([jnp.ones((NODES, 1), jnp.float32), node_points], axis=1)
    blocks = NODES // 16
    coeff_blocks = coefficients.reshape(blocks, 16, DIMS + 1)
    weight_blocks = weight.reshape(blocks, 16)

    def accumulate(carry, pieces):
        state = evolve(pieces[0], field_modes)
        first = carry[0] + jnp.einsum("b,bxy->xy", pieces[1], state, precision=lax.Precision.HIGHEST)
        second = carry[1] + jnp.einsum("b,bxy->xy", pieces[1], state * state, precision=lax.Precision.HIGHEST)
        return (first, second), None

    start = (jnp.zeros((NX, NY), jnp.float32), jnp.zeros((NX, NY), jnp.float32))
    (first, second), unused = lax.scan(accumulate, start, (coeff_blocks, weight_blocks))
    mean_field = first / weight_total
    variance_field = second / weight_total - mean_field * mean_field
    return mean_field, variance_field
```

```python
import functools

import jax
import jax.numpy as jnp
from jax import lax
from jax.experimental import pallas as pl
from jax.experimental.pallas import tpu as pltpu
from jax.sharding import PartitionSpec as P

TIME_STEP = 0.15
HALO = 4
LANES = 128
SUBLANES = 8
SLOTS = 256
MESH = pl.DeviceIdType.MESH
F32 = jnp.float32
BF16 = jnp.bfloat16


def nn(a, b):
    return lax.dot_general(a, b, (((1,), (0,)), ((), ())), preferred_element_type=F32)


def nt(a, b):
    return lax.dot_general(a, b, (((1,), (1,)), ((), ())), preferred_element_type=F32)


def split2(x):
    hi = x.astype(BF16).astype(F32)
    return hi, x - hi


def split3(x):
    hi = x.astype(BF16).astype(F32)
    rest = x - hi
    mid = rest.astype(BF16).astype(F32)
    return hi, mid, rest - mid


def kernel(
    gx_size, gy_size, rows, dims,
    field_hbm, points_ref, weight_ref, group_ref,
    total_ref, wsum_ref,
    fv, send_rows, recv_rows, send_cols, recv_cols, lhs, cols_t, rhs, node_w,
    cf0, cf1, u0a, u0b, u1, u2, u3, part, acc, nat, mine, theirs, csc,
    load_sem, send_sem, recv_sem,
):
    ext = rows + 2 * HALO
    pairs = ext // 2
    modes = dims + 1
    fields = 4 * modes
    ring = LANES + 2 * HALO
    chunk = ring // SUBLANES
    kpad = 40
    core = lax.axis_index("nodes")
    gx = lax.axis_index("gx")
    gy = lax.axis_index("gy")
    xn, xp = lax.rem(gx + 1, gx_size), lax.rem(gx + gx_size - 1, gx_size)
    yn, yp = lax.rem(gy + 1, gy_size), lax.rem(gy + gy_size - 1, gy_size)
    around = [
        (core, xp, gy), (core, xn, gy), (core, gx, yp), (core, gx, yn),
        (core, xp, yp), (core, xp, yn), (core, xn, yp), (core, xn, yn),
        (1 - core, gx, gy),
    ]

    load = pltpu.make_async_copy(field_hbm, fv.at[pl.ds(0, fields * rows)], load_sem)
    load.start()
    barrier = pltpu.get_barrier_semaphore()
    for device in around:
        pl.semaphore_signal(barrier, inc=1, device_id=device, device_id_type=MESH)

    fv[pl.ds(fields * rows, (kpad - fields) * rows), :] = jnp.zeros(((kpad - fields) * rows, LANES), F32)
    load.wait()

    for r in range(HALO):
        send_rows[0, pl.ds(r, kpad, stride=HALO), :] = fv[pl.ds(r, kpad, stride=rows), :]
        send_rows[1, pl.ds(r, kpad, stride=HALO), :] = fv[pl.ds(rows - HALO + r, kpad, stride=rows), :]
    lane = lax.broadcasted_iota(jnp.int32, (kpad, LANES), 1)
    per_tile = LANES // HALO
    tiles = rows // per_tile
    for t in range(tiles):
        low = jnp.zeros((kpad, LANES), F32)
        high = jnp.zeros((kpad, LANES), F32)
        for g in range(per_tile):
            x = fv[pl.ds(t * per_tile + g, kpad, stride=rows), :]
            x = pltpu.roll(x, (HALO * (g + 1)) % LANES, 1)
            high = jnp.where(lane // HALO == g, x, high)
            low = jnp.where(lane // HALO == (g + 1) % per_tile, x, low)
        send_cols[0, t] = low
        send_cols[1, t] = high

    pl.semaphore_wait(barrier, len(around))

    def remote(index, source, target, device):
        copy = pltpu.make_async_remote_copy(
            src_ref=source, dst_ref=target,
            send_sem=send_sem.at[index], recv_sem=recv_sem.at[index],
            device_id=device, device_id_type=MESH,
        )
        copy.start()
        return copy

    last = tiles - 1
    copies = [
        remote(2, send_cols.at[0], recv_cols.at[pl.ds(0, tiles)], (core, gx, yp)),
        remote(3, send_cols.at[1], recv_cols.at[pl.ds(tiles, tiles)], (core, gx, yn)),
        remote(0, send_rows.at[0], recv_rows.at[0], (core, xp, gy)),
        remote(1, send_rows.at[1], recv_rows.at[1], (core, xn, gy)),
        remote(4, send_cols.at[0, 0], recv_cols.at[2 * tiles], (core, xp, yp)),
        remote(5, send_cols.at[1, 0], recv_cols.at[2 * tiles + 1], (core, xp, yn)),
        remote(6, send_cols.at[0, last], recv_cols.at[2 * tiles + 2], (core, xn, yp)),
        remote(7, send_cols.at[1, last], recv_cols.at[2 * tiles + 3], (core, xn, yn)),
    ]

    count = group_ref.shape[1]
    included = (group_ref[...] < 2).astype(F32)
    weights = weight_ref[...]
    wsum_ref[...] = jnp.broadcast_to(jnp.sum(weights * included, axis=1, keepdims=True), wsum_ref.shape)
    before = lax.broadcasted_iota(jnp.int32, (count, count), 0) <= lax.broadcasted_iota(jnp.int32, (count, count), 1)
    order = nn(jnp.broadcast_to(included, (SUBLANES, count)).astype(BF16), before.astype(F32).astype(BF16))[0:1]
    slot = (lax.broadcasted_iota(jnp.int32, (SLOTS, count), 0) + (core * SLOTS + 1)).astype(F32)
    chosen = jnp.where(slot == jnp.broadcast_to(order, (SLOTS, count)), jnp.broadcast_to(included, (SLOTS, count)), 0.0)
    select = chosen.astype(BF16)
    eye = (
        lax.broadcasted_iota(jnp.int32, (SUBLANES, dims), 0) == lax.broadcasted_iota(jnp.int32, (SUBLANES, dims), 1)
    ).astype(F32).astype(BF16)
    coords = jnp.zeros((SUBLANES, SLOTS), F32)
    for piece in split3(points_ref[...]):
        picked = nn(select, piece.astype(BF16))
        coords = coords + nt(eye, picked.astype(BF16))
    held = jnp.zeros((SUBLANES, SLOTS), F32)
    for piece in split3(weights):
        held = held + nt(jnp.broadcast_to(piece, (SUBLANES, count)).astype(BF16), select)
    node_w[...] = held

    csc[...] = jnp.zeros_like(csc)
    csc[0:1, :] = jnp.ones((1, SLOTS), F32)
    csc[1 : 1 + dims, :] = coords
    coefficient = csc[...][0:modes]
    rhs[...] = jnp.zeros_like(rhs)

    def place(output, field, scale):
        hi, lo = split2(coefficient * scale)
        for h in range(2):
            lanes = pl.ds((output % 2) * LANES, LANES)
            at = field * modes
            part_hi = hi[:, h * LANES : (h + 1) * LANES]
            part_lo = lo[:, h * LANES : (h + 1) * LANES]
            rhs[h, output // 2, pl.ds(at, modes), lanes] = part_hi
            rhs[h, output // 2, pl.ds(kpad + at, modes), lanes] = part_lo
            rhs[h, output // 2, pl.ds(2 * kpad + at, modes), lanes] = part_hi

    diffuse, move = TIME_STEP, 0.5 * TIME_STEP
    for output, (field, sign) in enumerate([(None, 0), (1, -1), (1, 1), (2, -1), (2, 1)]):
        place(output, 3, -4.0 * diffuse if field is None else diffuse)
        if field is not None:
            place(output, field, sign * move)
    place(5, 0, 1.0)
    rhs[0, 0, 3 * kpad : 3 * kpad + 1, 0:LANES] = jnp.ones((1, LANES), F32)
    rhs[1, 0, 3 * kpad : 3 * kpad + 1, 0:LANES] = jnp.ones((1, LANES), F32)

    ones = jnp.where(lax.broadcasted_iota(jnp.int32, (SUBLANES, LANES), 0) == 0, 1.0, 0.0)

    def turned(x):
        hi, lo = split2(x)
        return jnp.transpose(jnp.concatenate([hi, hi, lo, ones], axis=0))

    @pl.loop(0, rows // 2)
    def _(pair):
        for half in range(2):
            row = 2 * pair + half
            at = pl.multiple_of((row + HALO) * ring, SUBLANES)
            lhs[pl.ds(at, LANES), :] = turned(fv[pl.ds(row, kpad, stride=rows), :])

    acc[...] = jnp.zeros_like(acc)

    for copy in copies:
        copy.wait_recv()

    for r in range(HALO):
        up = turned(recv_rows[1, pl.ds(r, kpad, stride=HALO), :])
        lhs[pl.ds(r * ring, LANES), :] = up
        down = turned(recv_rows[0, pl.ds(r, kpad, stride=HALO), :])
        lhs[pl.ds((rows + HALO + r) * ring, LANES), :] = down
    for t in range(2 * tiles + 4):
        cols_t[pl.ds(t * LANES, LANES), :] = turned(recv_cols[t])

    def column_halo(row, right, left):
        base = row * ring + LANES
        lhs[pl.ds(base, HALO), :] = cols_t[pl.ds(right, HALO), :]
        lhs[pl.ds(base + HALO, HALO), :] = cols_t[pl.ds(left, HALO), :]

    for row in range(rows):
        t, g = divmod(row, per_tile)
        column_halo(
            row + HALO,
            t * LANES + HALO * ((g + 1) % per_tile),
            (tiles + t) * LANES + HALO * g,
        )
    for r in range(HALO):
        corner = 2 * tiles * LANES
        column_halo(rows + HALO + r, corner + HALO * (r + 1), corner + LANES + HALO * r)
        g = per_tile - HALO + r
        column_halo(r, corner + 2 * LANES + HALO * ((g + 1) % per_tile), corner + 3 * LANES + HALO * g)

    cfs = (cf0, cf1)
    u0s = (u0a, u0b)
    states = (u0s, (u1.at[0], u1.at[1]), (u2.at[0], u2.at[1]), (u3.at[0], u3.at[1]))
    cf_ring, u_ring = cf0.shape[1], u0a.shape[0]

    def parameters(h, pair):
        pieces = []
        for half in range(2):
            base = (2 * pair + half) * ring
            pieces += [lhs[pl.ds(base + j, SUBLANES, stride=chunk), :] for j in range(chunk)]
        left = jnp.concatenate(pieces, axis=0)
        cslot = lax.rem(2 * pair, cf_ring)
        uslot = lax.rem(2 * pair, u_ring)
        for g in range(3):
            found = nn(left, rhs[h, g])
            for half in range(2):
                cut = found[half * ring : (half + 1) * ring]
                cfs[h][2 * g, cslot + half] = cut[:, 0:LANES]
                if g < 2:
                    cfs[h][2 * g + 1, cslot + half] = cut[:, LANES:]
                else:
                    u0s[h][uslot + half] = cut[:, LANES:]

    lane_of = lax.broadcasted_iota(jnp.int32, (SUBLANES, LANES), 1)
    tile = [pl.ds(SUBLANES * j, SUBLANES) for j in range(chunk)]

    def advance(step, h, pair):
        source = states[step - 1][h]
        slots = [lax.rem(2 * pair + u_ring - 1 + k, u_ring) for k in range(4)]
        cslot = lax.rem(2 * pair, cf_ring)
        below = [source[slots[0], tile[j], :] for j in range(chunk)]
        here = [source[slots[1], tile[j], :] for j in range(chunk)]
        for half in range(2):
            above = [source[slots[half + 2], tile[j], :] for j in range(chunk)]
            for j in range(chunk):
                north = here[j + 1] if j + 1 < chunk else pltpu.roll(here[0], SUBLANES - 1, 0)
                south = here[j - 1] if j else pltpu.roll(here[chunk - 1], 1, 0)
                c = [cfs[h][k, cslot + half, tile[j], :] for k in range(5)]
                new = (c[0] * here[j] + c[1] * above[j]) + c[2] * below[j] + (c[3] * north + c[4] * south)
                if step < 4:
                    states[step][h][slots[1 + half], tile[j], :] = new
                    continue
                w = node_w[:, h * LANES : (h + 1) * LANES]
                one = w * new
                two = one * new
                if h == 0:
                    part[half, 0, tile[j], :] = one
                    part[half, 1, tile[j], :] = two
                else:
                    row = 2 * pair + half - HALO
                    one = jnp.sum(one + part[half, 0, tile[j], :], axis=1, keepdims=True)
                    two = jnp.sum(two + part[half, 1, tile[j], :], axis=1, keepdims=True)
                    old = acc[tile[j], :]
                    old = jnp.where(lane_of == row, one, old)
                    acc[tile[j], :] = jnp.where(lane_of == row + rows, two, old)
            below, here = here, above

    lag = 2
    for pair in range(2):
        for h in range(2):
            parameters(h, pair)

    spans = {
        0: (0, pairs - 2),
        1: (0, pairs),
        2: (1 + lag, pairs - 1 + lag),
        3: (1 + 2 * lag, pairs - 1 + 2 * lag),
        4: (2 + 3 * lag, pairs - 2 + 3 * lag),
    }
    cuts = sorted({x for span in spans.values() for x in span})
    for first, final in zip(cuts[:-1], cuts[1:]):
        active = [k for k, (a, b) in spans.items() if a <= first and final <= b]

        @pl.loop(first, final)
        def _(q):
            for h in range(2):
                for step in (4, 3, 2, 1):
                    if step in active:
                        advance(step, h, q - lag * (step - 1))
                if 0 in active:
                    parameters(1 - h, q + 2)

    for j in range(chunk):
        nat[pl.ds(j, SUBLANES, stride=chunk), :] = acc[tile[j], :]
    mine[...] = jnp.transpose(nat[0:LANES, :])
    swap = remote(8, mine, theirs, (1 - core, gx, gy))
    for copy in copies:
        copy.wait_send()
    swap.wait()
    total_ref[...] = mine[...] + theirs[...]


def on_device(mesh, field_modes, node_points, quad_weight, group_of):
    rows, cols = field_modes.shape[2:]
    count, dims = node_points.shape
    modes = dims + 1
    ext = rows + 2 * HALO
    ring = cols + 2 * HALO
    kpad = 40
    tiles = rows * HALO // LANES
    vmem = pl.BlockSpec(memory_space=pltpu.VMEM)
    total, wsum = pl.pallas_call(
        functools.partial(kernel, mesh.shape["gx"], mesh.shape["gy"], rows, dims),
        out_shape=(
            jax.ShapeDtypeStruct((2 * rows, cols), F32),
            jax.ShapeDtypeStruct((SUBLANES, LANES), F32),
        ),
        in_specs=[pl.BlockSpec(memory_space=pl.ANY), vmem, vmem, vmem],
        out_specs=(vmem, vmem),
        scratch_shapes=[
            pltpu.VMEM((kpad * rows, LANES), F32),
            pltpu.VMEM((2, kpad * HALO, LANES), F32),
            pltpu.VMEM((2, kpad * HALO, LANES), F32),
            pltpu.VMEM((2, tiles, kpad, LANES), F32),
            pltpu.VMEM((2 * tiles + 4, kpad, LANES), F32),
            pltpu.VMEM((ext * ring, LANES), F32),
            pltpu.VMEM(((2 * tiles + 4) * LANES, LANES), F32),
            pltpu.VMEM((2, 3, LANES, 2 * LANES), F32),
            pltpu.VMEM((SUBLANES, SLOTS), F32),
            pltpu.VMEM((5, 32, ring, LANES), F32),
            pltpu.VMEM((5, 32, ring, LANES), F32),
            pltpu.VMEM((8, ring, LANES), F32),
            pltpu.VMEM((8, ring, LANES), F32),
            pltpu.VMEM((2, 8, ring, LANES), F32),
            pltpu.VMEM((2, 8, ring, LANES), F32),
            pltpu.VMEM((2, 8, ring, LANES), F32),
            pltpu.VMEM((2, 2, ring, LANES), F32),
            pltpu.VMEM((ring, LANES), F32),
            pltpu.VMEM((ring, LANES), F32),
            pltpu.VMEM((2 * rows, LANES), F32),
            pltpu.VMEM((2 * rows, LANES), F32),
            pltpu.VMEM((2 * SUBLANES, SLOTS), F32),
            pltpu.SemaphoreType.DMA,
            pltpu.SemaphoreType.DMA((9,)),
            pltpu.SemaphoreType.DMA((9,)),
        ],
        compiler_params=pltpu.CompilerParams(
            collective_id=0, has_side_effects=True, vmem_limit_bytes=60 * 1024 * 1024
        ),
    )(
        field_modes.reshape(4 * modes * rows, cols),
        node_points,
        quad_weight.reshape(1, count),
        group_of.reshape(1, count),
    )
    weight_total = wsum[0, 0]
    mean_field = total[:rows] / weight_total
    variance_field = total[rows:] / weight_total - mean_field * mean_field
    return mean_field, variance_field


def solution(mesh):
    return jax.shard_map(
        functools.partial(on_device, mesh),
        mesh=mesh,
        in_specs=(P(None, None, "gx", "gy"), P(), P(), P()),
        out_specs=(P("gx", "gy"), P("gx", "gy")),
        check_vma=False,
    )
```

```python
import functools

import jax
import jax.numpy as jnp
from jax import lax
from jax.experimental import pallas as pl
from jax.experimental.pallas import tpu as pltpu
from jax.sharding import PartitionSpec as P

TIME_STEP = 0.15
HALO = 4
LANES = 128
SUBLANES = 8
SLOTS = 256
ROWS = 4
MESH = pl.DeviceIdType.MESH
F32 = jnp.float32
BF16 = jnp.bfloat16


def nn(a, b):
    return lax.dot_general(a, b, (((1,), (0,)), ((), ())), preferred_element_type=F32)


def nt(a, b):
    return lax.dot_general(a, b, (((1,), (1,)), ((), ())), preferred_element_type=F32)


def split2(x):
    hi = x.astype(BF16).astype(F32)
    return hi, x - hi


def split3(x):
    hi = x.astype(BF16).astype(F32)
    rest = x - hi
    mid = rest.astype(BF16).astype(F32)
    return hi, mid, rest - mid


def kernel(
    gx_size, gy_size, rows, dims,
    field_hbm, points_ref, weight_ref, group_ref,
    moments_ref,
    fv, send_rows, recv_rows, send_cols, recv_cols, send_corners, recv_corners,
    lnat, left, cols_t, halo_l, rhs_f, rhs, node_w, csc,
    cf0, cf1, ua, ub, kept, part, both, acc, nat, mine, theirs,
    load_sem, send_sem, recv_sem,
):
    ext = rows + 2 * HALO
    quads = ext // ROWS
    modes = dims + 1
    fields = 4 * modes
    ring = LANES + 2 * HALO
    chunk = ring // SUBLANES
    kpad = 40
    groups = kpad // SUBLANES
    core = lax.axis_index("nodes")
    gx = lax.axis_index("gx")
    gy = lax.axis_index("gy")
    xn, xp = lax.rem(gx + 1, gx_size), lax.rem(gx + gx_size - 1, gx_size)
    yn, yp = lax.rem(gy + 1, gy_size), lax.rem(gy + gy_size - 1, gy_size)
    around = [
        (core, xp, gy), (core, xn, gy), (core, gx, yp), (core, gx, yn),
        (core, xp, yp), (core, xp, yn), (core, xn, yp), (core, xn, yn),
        (1 - core, gx, gy),
    ]

    load = pltpu.make_async_copy(field_hbm, fv.at[pl.ds(0, fields * rows)], load_sem)
    load.start()
    barrier = pltpu.get_barrier_semaphore()
    for device in around:
        pl.semaphore_signal(barrier, inc=1, device_id=device, device_id_type=MESH)

    fv[pl.ds(fields * rows, (kpad - fields) * rows), :] = jnp.zeros(((kpad - fields) * rows, LANES), F32)
    load.wait()

    for r in range(HALO):
        send_rows[0, pl.ds(r, kpad, stride=HALO), :] = fv[pl.ds(r, kpad, stride=rows), :]
        send_rows[1, pl.ds(r, kpad, stride=HALO), :] = fv[pl.ds(rows - HALO + r, kpad, stride=rows), :]
    lane = lax.broadcasted_iota(jnp.int32, (SUBLANES, LANES), 1)
    by_halo = lane // HALO
    block = HALO * HALO
    by_block = lane // block
    per_tile = LANES // HALO
    tiles = rows // per_tile
    for t in range(tiles):
        low = [jnp.zeros((SUBLANES, LANES), F32)] * groups
        high = [jnp.zeros((SUBLANES, LANES), F32)] * groups
        for g in range(per_tile):
            at_high = by_halo == g
            at_low = by_halo == (g + 1) % per_tile
            for m in range(groups):
                x = fv[pl.ds(m * SUBLANES * rows + t * per_tile + g, SUBLANES, stride=rows), :]
                x = pltpu.roll(x, (HALO * (g + 1)) % LANES, 1)
                high[m] = jnp.where(at_high, x, high[m])
                low[m] = jnp.where(at_low, x, low[m])
        for side, values in enumerate((low, high)):
            for m in range(groups):
                send_cols[side, t, m * SUBLANES : (m + 1) * SUBLANES, :] = values[m]
            for end in range(2):
                if t != (0, tiles - 1)[end]:
                    continue
                at = HALO * (1 - side) + (0, LANES - block)[end]
                packed = jnp.zeros((SUBLANES, LANES), F32)
                for m in range(groups):
                    packed = jnp.where(by_block == m, pltpu.roll(values[m], (block * m - at) % LANES, 1), packed)
                send_corners[2 * end + side] = packed

    pl.semaphore_wait(barrier, len(around))

    def remote(index, source, target, device):
        copy = pltpu.make_async_remote_copy(
            src_ref=source, dst_ref=target,
            send_sem=send_sem.at[index], recv_sem=recv_sem.at[index],
            device_id=device, device_id_type=MESH,
        )
        copy.start()
        return copy

    sent = fields * HALO
    copies = [
        remote(0, send_rows.at[0, pl.ds(0, sent)], recv_rows.at[0, pl.ds(0, sent)], (core, xp, gy)),
        remote(1, send_rows.at[1, pl.ds(0, sent)], recv_rows.at[1, pl.ds(0, sent)], (core, xn, gy)),
        remote(2, send_cols.at[0], recv_cols.at[0], (core, gx, yp)),
        remote(3, send_cols.at[1], recv_cols.at[1], (core, gx, yn)),
        remote(4, send_corners.at[0], recv_corners.at[0], (core, xp, yp)),
        remote(5, send_corners.at[1], recv_corners.at[1], (core, xp, yn)),
        remote(6, send_corners.at[2], recv_corners.at[2], (core, xn, yp)),
        remote(7, send_corners.at[3], recv_corners.at[3], (core, xn, yn)),
    ]

    count = group_ref.shape[0]
    included = (group_ref[...].reshape(1, count) < 2).astype(F32)
    weights = weight_ref[...].reshape(1, count)
    weight_total = jnp.sum(weights * included, axis=1, keepdims=True)
    row8 = lax.broadcasted_iota(jnp.int32, (SUBLANES, LANES), 0)
    blocks = count // LANES
    pieces = [included[:, b * LANES : (b + 1) * LANES] for b in range(blocks)]
    stacked = jnp.zeros((SUBLANES, LANES), F32)
    for b in range(blocks):
        stacked = jnp.where(row8 == b, jnp.broadcast_to(pieces[b], (SUBLANES, LANES)), stacked)
    before = lax.broadcasted_iota(jnp.int32, (LANES, LANES), 0) <= lax.broadcasted_iota(jnp.int32, (LANES, LANES), 1)
    within = nn(stacked.astype(BF16), before.astype(F32).astype(BF16))
    totals = jnp.sum(stacked, axis=1, keepdims=True)
    slot = (lax.broadcasted_iota(jnp.int32, (SLOTS, LANES), 0) + (core * SLOTS + 1)).astype(F32)
    offset = jnp.zeros((1, 1), F32)
    chosen = []
    for b in range(blocks):
        order = within[b : b + 1] + offset
        offset = offset + totals[b : b + 1]
        order = jnp.where(pieces[b] > 0, order, 0.0)
        chosen.append(jnp.where(slot == jnp.broadcast_to(order, (SLOTS, LANES)), 1.0, 0.0).astype(BF16))
    select = jnp.concatenate(chosen, axis=1)
    w_hi, w_mid, w_lo = split3(weights)
    w_rows = lax.broadcasted_iota(jnp.int32, (SUBLANES, count), 0)
    w_stack = jnp.where(w_rows == 0, w_hi, jnp.where(w_rows == 1, w_mid, jnp.where(w_rows == 2, w_lo, 0.0)))
    found = nt(jnp.concatenate([*split3(points_ref[...]), w_stack], axis=0).astype(BF16), select)
    coords = found[0:dims] + found[dims : 2 * dims] + found[2 * dims : 3 * dims]
    held = found[3 * dims : 3 * dims + 1] + found[3 * dims + 1 : 3 * dims + 2] + found[3 * dims + 2 : 3 * dims + 3]
    node_w[...] = jnp.broadcast_to(held, (SUBLANES, SLOTS))

    csc[0:1, :] = jnp.ones((1, SLOTS), F32)
    csc[1 : 1 + dims, :] = coords
    coefficient = csc[...][0:modes]
    rhs_f[...] = jnp.zeros_like(rhs_f)

    def place(group, half, h, field, scale):
        hi, lo = split2(coefficient[:, h * LANES : (h + 1) * LANES] * scale)
        at = field * modes
        lanes = pl.ds(half * LANES, LANES)
        rhs_f[group, pl.ds(at, modes), lanes] = hi
        rhs_f[group, pl.ds(kpad + at, modes), lanes] = lo
        rhs_f[group, pl.ds(2 * kpad + at, modes), lanes] = hi

    for h in range(2):
        for k in range(4):
            place(2 * h + k // 2, k % 2, h, 3, TIME_STEP)
            place(2 * h + k // 2, k % 2, h, 1 + k // 2, (-0.5, 0.5)[k % 2] * TIME_STEP)
        place(4, h, h, 0, 1.0)
    rhs[...] = rhs_f[...].astype(BF16)

    rest = jnp.zeros((SUBLANES, LANES), F32)

    def turned(x):
        hi, lo = split2(x)
        stack = jnp.concatenate([hi, hi, lo, rest], axis=0).astype(BF16)
        return jnp.transpose(stack).astype(F32)

    def turn_rows(quad):
        for k in range(ROWS):
            x = fv[pl.ds(ROWS * quad - HALO + k, kpad, stride=rows), :]
            lnat[lax.rem(quad, 2), pl.ds(k * ring, LANES), :] = turned(x)

    cfs, us = (cf0, cf1), (ua, ub)

    def targets(group):
        if group == 4:
            return [lambda row: us[0].at[row], lambda row: us[1].at[row]]
        return [
            lambda row: cfs[group // 2].at[row, 2 * (group % 2)],
            lambda row: cfs[group // 2].at[row, 2 * (group % 2) + 1],
        ]

    def parameters(quad):
        slot = lax.rem(quad, 2)
        cells = []
        for k in range(ROWS):
            cells += [lnat[slot, pl.ds(k * ring + j, SUBLANES, stride=chunk), :] for j in range(chunk)]
        left[...] = jnp.concatenate(cells, axis=0).astype(BF16)
        for group in range(5):
            found = nn(left[...], rhs[group])
            for half, target in enumerate(targets(group)):
                for k in range(ROWS):
                    piece = found[k * ring : (k + 1) * ring, half * LANES : (half + 1) * LANES]
                    target(ROWS * quad + k)[...] = piece

    for side in range(2):
        recv_rows[side, pl.ds(sent, kpad * HALO - sent), :] = jnp.zeros((kpad * HALO - sent, LANES), F32)
    acc[...] = jnp.zeros_like(acc)

    turn_rows(1)

    @pl.loop(1, quads - 2)
    def _(quad):
        parameters(quad)
        turn_rows(quad + 1)

    parameters(quads - 2)

    for copy in copies:
        copy.wait_recv()

    for side, quad in ((1, 0), (0, quads - 1)):
        for k in range(ROWS):
            x = recv_rows[side, pl.ds(k, kpad, stride=HALO), :]
            lnat[quad % 2, pl.ds(k * ring, LANES), :] = turned(x)
        parameters(quad)

    for t in range(2 * tiles):
        cols_t[pl.ds(t * LANES, LANES), :] = turned(recv_cols[t // tiles, t % tiles])
    corners = [recv_corners[k] for k in range(4)]
    unpacked = []
    for m in range(groups):
        x = jnp.zeros((SUBLANES, LANES), F32)
        for k in range(4):
            x = jnp.where(by_block == k, pltpu.roll(corners[k], block * (k - m) % LANES, 1), x)
        unpacked.append(x)
    cols_t[pl.ds(2 * tiles * LANES, LANES), :] = turned(jnp.concatenate(unpacked, axis=0))

    def column_halo(row, right, left_side):
        halo_l[pl.ds(row * SUBLANES, HALO), :] = cols_t[pl.ds(right, HALO), :]
        halo_l[pl.ds(row * SUBLANES + HALO, HALO), :] = cols_t[pl.ds(left_side, HALO), :]

    for row in range(rows):
        t, g = divmod(row, per_tile)
        column_halo(
            row + HALO,
            t * LANES + HALO * ((g + 1) % per_tile),
            (tiles + t) * LANES + HALO * g,
        )
    corner = 2 * tiles * LANES
    for r in range(HALO):
        column_halo(rows + HALO + r, corner + HALO * r, corner + block + HALO * r)
        column_halo(r, corner + 2 * block + HALO * r, corner + 3 * block + HALO * r)
    edge = (chunk - SUBLANES) * SUBLANES + SUBLANES - 1
    for group in range(5):
        found = nn(halo_l[...].astype(BF16), rhs[group])
        for half, target in enumerate(targets(group)):
            for row in range(ext):
                piece = found[row * SUBLANES : (row + 1) * SUBLANES, half * LANES : (half + 1) * LANES]
                target(row)[pl.ds(edge, SUBLANES, stride=SUBLANES), :] = piece

    tile = [pl.ds(SUBLANES * j, SUBLANES) for j in range(chunk)]

    def advance(step, h, first):
        cf = cfs[h].at[pl.ds(first, ROWS)]
        u = us[h].at[pl.ds(first, ROWS + 1)]
        cells = [kept.at[h]] + [u.at[k] for k in range(ROWS + 1)]

        def column(j):
            return [ref[tile[j], :] for ref in cells]

        column_now = column(0)
        last = [ref[tile[chunk - 1], :] for ref in cells[1:-1]]
        wrap = [column_now[k + 1] - pltpu.roll(last[k], 1, 0) for k in range(ROWS)]
        south = wrap
        for j in range(chunk):
            if j + 1 < chunk:
                column_next = column(j + 1)
                north = [column_next[k + 1] - column_now[k + 1] for k in range(ROWS)]
            else:
                column_next = None
                north = [pltpu.roll(x, SUBLANES - 1, 0) for x in wrap]
            east = [column_now[k + 1] - column_now[k] for k in range(ROWS + 1)]
            for k in range(ROWS):
                c = [cf[k, m, tile[j], :] for m in range(4)]
                new = column_now[k + 1] + (
                    (c[0] * east[k + 1] - c[1] * east[k]) + (c[2] * north[k] - c[3] * south[k])
                )
                if step < 4:
                    u[k, tile[j], :] = new
                    continue
                one = node_w[:, h * LANES : (h + 1) * LANES] * new
                two = one * new
                if h == 0:
                    part[k, 0, tile[j], :] = one
                    part[k, 1, tile[j], :] = two
                else:
                    both[k, 0, tile[j], :] = one + part[k, 0, tile[j], :]
                    both[k, 1, tile[j], :] = two + part[k, 1, tile[j], :]
            kept[h, tile[j], :] = column_now[ROWS]
            column_now, south = column_next, north

    def gather_sums(first):
        masks = [(lane == first + k + m * rows, k, m) for k in range(ROWS) for m in range(2)]
        for j in range(chunk):
            old = acc[tile[j], :]
            for mask, k, m in masks:
                old = jnp.where(mask, jnp.sum(both[k, m, tile[j], :], axis=1, keepdims=True), old)
            acc[tile[j], :] = old

    for step, (start, turns) in {1: (0, quads), 2: (2, quads - 1), 3: (1, quads - 1), 4: (HALO, quads - 2)}.items():
        for h in range(2):
            kept[h] = us[h][max(start - 1, 0)]
        if step == 4:
            both[...] = jnp.zeros_like(both)

        @pl.loop(0, turns)
        def _(turn):
            first = start + ROWS * turn
            if step == 4:
                gather_sums(first - HALO - ROWS)
            for h in range(2):
                advance(step, h, first)

    gather_sums(rows - ROWS)

    for j in range(chunk):
        nat[pl.ds(j, SUBLANES, stride=chunk), :] = acc[tile[j], :]
    mine[...] = jnp.transpose(nat[0:LANES, :])
    swap = remote(8, mine, theirs, (1 - core, gx, gy))
    for copy in copies:
        copy.wait_send()
    swap.wait()
    moments_ref[...] = (mine[...] + theirs[...]) / weight_total


def on_device(mesh, field_modes, node_points, quad_weight, group_of):
    rows, cols = field_modes.shape[2:]
    count, dims = node_points.shape
    modes = dims + 1
    ext = rows + 2 * HALO
    ring = cols + 2 * HALO
    kpad = 40
    tiles = rows * HALO // LANES
    vmem = pl.BlockSpec(memory_space=pltpu.VMEM)
    moments = pl.pallas_call(
        functools.partial(kernel, mesh.shape["gx"], mesh.shape["gy"], rows, dims),
        out_shape=jax.ShapeDtypeStruct((2 * rows, cols), F32),
        in_specs=[pl.BlockSpec(memory_space=pl.ANY), vmem, vmem, vmem],
        out_specs=vmem,
        scratch_shapes=[
            pltpu.VMEM((kpad * rows, LANES), F32),
            pltpu.VMEM((2, kpad * HALO, LANES), F32),
            pltpu.VMEM((2, kpad * HALO, LANES), F32),
            pltpu.VMEM((2, tiles, kpad, LANES), F32),
            pltpu.VMEM((2, tiles, kpad, LANES), F32),
            pltpu.VMEM((4, SUBLANES, LANES), F32),
            pltpu.VMEM((4, SUBLANES, LANES), F32),
            pltpu.VMEM((2, ROWS * ring, LANES), F32),
            pltpu.VMEM((ROWS * ring, LANES), BF16),
            pltpu.VMEM(((2 * tiles + 1) * LANES, LANES), F32),
            pltpu.VMEM((ext * SUBLANES, LANES), F32),
            pltpu.VMEM((5, LANES, 2 * LANES), F32),
            pltpu.VMEM((5, LANES, 2 * LANES), BF16),
            pltpu.VMEM((SUBLANES, SLOTS), F32),
            pltpu.VMEM((2 * SUBLANES, SLOTS), F32),
            pltpu.VMEM((ext, 4, ring, LANES), F32),
            pltpu.VMEM((ext, 4, ring, LANES), F32),
            pltpu.VMEM((ext + 1, ring, LANES), F32),
            pltpu.VMEM((ext + 1, ring, LANES), F32),
            pltpu.VMEM((2, ring, LANES), F32),
            pltpu.VMEM((ROWS, 2, ring, LANES), F32),
            pltpu.VMEM((ROWS, 2, ring, LANES), F32),
            pltpu.VMEM((ring, LANES), F32),
            pltpu.VMEM((ring, LANES), F32),
            pltpu.VMEM((2 * rows, LANES), F32),
            pltpu.VMEM((2 * rows, LANES), F32),
            pltpu.SemaphoreType.DMA,
            pltpu.SemaphoreType.DMA((9,)),
            pltpu.SemaphoreType.DMA((9,)),
        ],
        compiler_params=pltpu.CompilerParams(
            collective_id=0, has_side_effects=True, vmem_limit_bytes=62 * 1024 * 1024
        ),
    )(
        field_modes.reshape(4 * modes * rows, cols),
        node_points.T,
        quad_weight,
        group_of,
    )
    mean_field = moments[:rows]
    return mean_field, moments[rows:] - mean_field * mean_field


def solution(mesh):
    return jax.shard_map(
        functools.partial(on_device, mesh),
        mesh=mesh,
        in_specs=(P(None, None, "gx", "gy"), P(), P(), P()),
        out_specs=(P("gx", "gy"), P("gx", "gy")),
        check_vma=False,
    )
```

```python
import functools

import jax
import jax.numpy as jnp
from jax import lax
from jax.experimental import pallas as pl
from jax.experimental.pallas import tpu as pltpu
from jax.sharding import PartitionSpec as P

TIME_STEP = 0.15
HALO = 4
LANES = 128
SUBLANES = 8
SLOTS = 256
ROWS = 4
MESH = pl.DeviceIdType.MESH
F32 = jnp.float32
BF16 = jnp.bfloat16


def nn(a, b):
    return lax.dot_general(a, b, (((1,), (0,)), ((), ())), preferred_element_type=F32)


def nt(a, b):
    return lax.dot_general(a, b, (((1,), (1,)), ((), ())), preferred_element_type=F32)


def split2(x):
    hi = x.astype(BF16).astype(F32)
    return hi, x - hi


def split3(x):
    hi = x.astype(BF16).astype(F32)
    rest = x - hi
    mid = rest.astype(BF16).astype(F32)
    return hi, mid, rest - mid


def kernel(
    gx_size, gy_size, rows, dims,
    field_hbm, points_hbm, weight_hbm, group_hbm,
    moments_ref,
    fv, send_rows, recv_rows, send_cols, recv_cols, send_corners, recv_corners,
    lnat, left, cols_t, halo_l, rhs_f, rhs, node_w, csc,
    cf0, cf1, ua, ub, kept, part, both, acc, nat, mine, theirs,
    points_ref, weight_ref, group_ref,
    load_sem, send_sem, recv_sem,
):
    ext = rows + 2 * HALO
    quads = ext // ROWS
    modes = dims + 1
    fields = 4 * modes
    ring = LANES + 2 * HALO
    chunk = ring // SUBLANES
    kpad = 40
    groups = kpad // SUBLANES
    core = lax.axis_index("nodes")
    gx = lax.axis_index("gx")
    gy = lax.axis_index("gy")
    xn, xp = lax.rem(gx + 1, gx_size), lax.rem(gx + gx_size - 1, gx_size)
    yn, yp = lax.rem(gy + 1, gy_size), lax.rem(gy + gy_size - 1, gy_size)
    around = [
        (core, xp, gy), (core, xn, gy), (core, gx, yp), (core, gx, yn),
        (core, xp, yp), (core, xp, yn), (core, xn, yp), (core, xn, yn),
        (1 - core, gx, gy),
    ]

    barrier = pltpu.get_barrier_semaphore()
    for device in around:
        pl.semaphore_signal(barrier, inc=1, device_id=device, device_id_type=MESH)

    apart = fv.shape[0] // kpad

    @pl.loop(0, fields)
    def _(k):
        pltpu.make_async_copy(
            field_hbm.at[pl.ds(k * rows, rows)], fv.at[pl.ds(k * apart, rows)], load_sem.at[0]
        ).start()

    small = [
        pltpu.make_async_copy(source, target, load_sem.at[1 + i])
        for i, (source, target) in enumerate(
            [(points_hbm, points_ref), (weight_hbm, weight_ref), (group_hbm, group_ref)]
        )
    ]
    for copy in small:
        copy.start()
    fv[pl.ds(fields * apart, (kpad - fields) * apart), :] = jnp.zeros(((kpad - fields) * apart, LANES), F32)
    pltpu.make_async_copy(field_hbm, fv.at[pl.ds(0, fields * rows)], load_sem.at[0]).wait()

    for r in range(HALO):
        send_rows[0, pl.ds(r, kpad, stride=HALO), :] = fv[pl.ds(r, kpad, stride=apart), :]
        send_rows[1, pl.ds(r, kpad, stride=HALO), :] = fv[pl.ds(rows - HALO + r, kpad, stride=apart), :]

    pl.semaphore_wait(barrier, len(around))

    def remote(index, source, target, device):
        copy = pltpu.make_async_remote_copy(
            src_ref=source, dst_ref=target,
            send_sem=send_sem.at[index], recv_sem=recv_sem.at[index],
            device_id=device, device_id_type=MESH,
        )
        copy.start()
        return copy

    sent = fields * HALO
    copies = [
        remote(0, send_rows.at[0, pl.ds(0, sent)], recv_rows.at[0, pl.ds(0, sent)], (core, xp, gy)),
        remote(1, send_rows.at[1, pl.ds(0, sent)], recv_rows.at[1, pl.ds(0, sent)], (core, xn, gy)),
    ]
    lane = lax.broadcasted_iota(jnp.int32, (SUBLANES, LANES), 1)
    by_halo = lane // HALO
    block = HALO * HALO
    by_block = lane // block
    per_tile = LANES // HALO
    tiles = rows // per_tile
    for t in range(tiles):
        low = [jnp.zeros((SUBLANES, LANES), F32)] * groups
        high = [jnp.zeros((SUBLANES, LANES), F32)] * groups
        for g in range(per_tile):
            at_high = by_halo == g
            at_low = by_halo == (g + 1) % per_tile
            for m in range(groups):
                x = fv[pl.ds(m * SUBLANES * apart + t * per_tile + g, SUBLANES, stride=apart), :]
                x = pltpu.roll(x, (HALO * (g + 1)) % LANES, 1)
                high[m] = jnp.where(at_high, x, high[m])
                low[m] = jnp.where(at_low, x, low[m])
        for side, values in enumerate((low, high)):
            for m in range(groups):
                send_cols[side, t, m * SUBLANES : (m + 1) * SUBLANES, :] = values[m]
            for end in range(2):
                if t != (0, tiles - 1)[end]:
                    continue
                at = HALO * (1 - side) + (0, LANES - block)[end]
                packed = jnp.zeros((SUBLANES, LANES), F32)
                for m in range(groups):
                    packed = jnp.where(by_block == m, pltpu.roll(values[m], (block * m - at) % LANES, 1), packed)
                send_corners[2 * end + side] = packed

    copies += [
        remote(2, send_cols.at[0], recv_cols.at[0], (core, gx, yp)),
        remote(3, send_cols.at[1], recv_cols.at[1], (core, gx, yn)),
        remote(4, send_corners.at[0], recv_corners.at[0], (core, xp, yp)),
        remote(5, send_corners.at[1], recv_corners.at[1], (core, xp, yn)),
        remote(6, send_corners.at[2], recv_corners.at[2], (core, xn, yp)),
        remote(7, send_corners.at[3], recv_corners.at[3], (core, xn, yn)),
    ]

    for copy in small:
        copy.wait()
    count = group_ref.shape[0]
    included = (group_ref[...].reshape(1, count) < 2).astype(F32)
    weights = weight_ref[...].reshape(1, count)
    weight_total = jnp.sum(weights * included, axis=1, keepdims=True)
    row8 = lax.broadcasted_iota(jnp.int32, (SUBLANES, LANES), 0)
    blocks = count // LANES
    pieces = [included[:, b * LANES : (b + 1) * LANES] for b in range(blocks)]
    stacked = jnp.zeros((SUBLANES, LANES), F32)
    for b in range(blocks):
        stacked = jnp.where(row8 == b, jnp.broadcast_to(pieces[b], (SUBLANES, LANES)), stacked)
    before = lax.broadcasted_iota(jnp.int32, (LANES, LANES), 0) <= lax.broadcasted_iota(jnp.int32, (LANES, LANES), 1)
    within = nn(stacked.astype(BF16), before.astype(F32).astype(BF16))
    totals = jnp.sum(stacked, axis=1, keepdims=True)
    slot = (lax.broadcasted_iota(jnp.int32, (SLOTS, LANES), 0) + (core * SLOTS + 1)).astype(F32)
    offset = jnp.zeros((1, 1), F32)
    chosen = []
    for b in range(blocks):
        order = within[b : b + 1] + offset
        offset = offset + totals[b : b + 1]
        order = jnp.where(pieces[b] > 0, order, 0.0)
        chosen.append(jnp.where(slot == jnp.broadcast_to(order, (SLOTS, LANES)), 1.0, 0.0).astype(BF16))
    select = jnp.concatenate(chosen, axis=1)
    w_hi, w_mid, w_lo = split3(weights)
    w_rows = lax.broadcasted_iota(jnp.int32, (SUBLANES, count), 0)
    w_stack = jnp.where(w_rows == 0, w_hi, jnp.where(w_rows == 1, w_mid, jnp.where(w_rows == 2, w_lo, 0.0)))
    found = nt(jnp.concatenate([*split3(points_ref[...]), w_stack], axis=0).astype(BF16), select)
    coords = found[0:dims] + found[dims : 2 * dims] + found[2 * dims : 3 * dims]
    held = found[3 * dims : 3 * dims + 1] + found[3 * dims + 1 : 3 * dims + 2] + found[3 * dims + 2 : 3 * dims + 3]
    node_w[...] = jnp.broadcast_to(held, (SUBLANES, SLOTS))

    csc[0:1, :] = jnp.ones((1, SLOTS), F32)
    csc[1 : 1 + dims, :] = coords
    coefficient = csc[...][0:modes]
    rhs_f[...] = jnp.zeros_like(rhs_f)

    def place(group, half, h, field, scale):
        hi, lo = split2(coefficient[:, h * LANES : (h + 1) * LANES] * scale)
        at = field * modes
        lanes = pl.ds(half * LANES, LANES)
        rhs_f[group, pl.ds(at, modes), lanes] = hi
        rhs_f[group, pl.ds(kpad + at, modes), lanes] = lo
        rhs_f[group, pl.ds(2 * kpad + at, modes), lanes] = hi

    for h in range(2):
        for k in range(4):
            place(2 * h + k // 2, k % 2, h, 3, TIME_STEP)
            place(2 * h + k // 2, k % 2, h, 1 + k // 2, (-0.5, 0.5)[k % 2] * TIME_STEP)
        place(4, h, h, 0, 1.0)
    rhs[...] = rhs_f[...].astype(BF16)

    rest = jnp.zeros((SUBLANES, LANES), F32)

    def turned(x):
        hi, lo = split2(x)
        stack = jnp.concatenate([hi, hi, lo, rest], axis=0).astype(BF16)
        return jnp.transpose(stack).astype(F32)

    def turn_rows(quad):
        for k in range(ROWS):
            x = fv[pl.ds(ROWS * quad - HALO + k, kpad, stride=apart), :]
            lnat[lax.rem(quad, 2), pl.ds(k * ring, LANES), :] = turned(x)

    cfs, us = (cf0, cf1), (ua, ub)

    def targets(group):
        if group == 4:
            return [lambda row: us[0].at[row], lambda row: us[1].at[row]]
        return [
            lambda row: cfs[group // 2].at[row, 2 * (group % 2)],
            lambda row: cfs[group // 2].at[row, 2 * (group % 2) + 1],
        ]

    def parameters(quad):
        slot = lax.rem(quad, 2)
        cells = []
        for k in range(ROWS):
            cells += [lnat[slot, pl.ds(k * ring + j, SUBLANES, stride=chunk), :] for j in range(chunk)]
        left[...] = jnp.concatenate(cells, axis=0).astype(BF16)
        for group in range(5):
            found = nn(left[...], rhs[group])
            for half, target in enumerate(targets(group)):
                for k in range(ROWS):
                    piece = found[k * ring : (k + 1) * ring, half * LANES : (half + 1) * LANES]
                    target(ROWS * quad + k)[...] = piece

    for side in range(2):
        recv_rows[side, pl.ds(sent, kpad * HALO - sent), :] = jnp.zeros((kpad * HALO - sent, LANES), F32)
    acc[...] = jnp.zeros_like(acc)

    turn_rows(1)

    @pl.loop(1, quads - 2)
    def _(quad):
        parameters(quad)
        turn_rows(quad + 1)

    parameters(quads - 2)

    for copy in copies:
        copy.wait_recv()

    for side, quad in ((1, 0), (0, quads - 1)):
        for k in range(ROWS):
            x = recv_rows[side, pl.ds(k, kpad, stride=HALO), :]
            lnat[quad % 2, pl.ds(k * ring, LANES), :] = turned(x)
        parameters(quad)

    for t in range(2 * tiles):
        cols_t[pl.ds(t * LANES, LANES), :] = turned(recv_cols[t // tiles, t % tiles])
    corners = [recv_corners[k] for k in range(4)]
    unpacked = []
    for m in range(groups):
        x = jnp.zeros((SUBLANES, LANES), F32)
        for k in range(4):
            x = jnp.where(by_block == k, pltpu.roll(corners[k], block * (k - m) % LANES, 1), x)
        unpacked.append(x)
    cols_t[pl.ds(2 * tiles * LANES, LANES), :] = turned(jnp.concatenate(unpacked, axis=0))

    def column_halo(row, right, left_side):
        halo_l[pl.ds(row * SUBLANES, HALO), :] = cols_t[pl.ds(right, HALO), :]
        halo_l[pl.ds(row * SUBLANES + HALO, HALO), :] = cols_t[pl.ds(left_side, HALO), :]

    for row in range(rows):
        t, g = divmod(row, per_tile)
        column_halo(
            row + HALO,
            t * LANES + HALO * ((g + 1) % per_tile),
            (tiles + t) * LANES + HALO * g,
        )
    corner = 2 * tiles * LANES
    for r in range(HALO):
        column_halo(rows + HALO + r, corner + HALO * r, corner + block + HALO * r)
        column_halo(r, corner + 2 * block + HALO * r, corner + 3 * block + HALO * r)
    edge = (chunk - SUBLANES) * SUBLANES + SUBLANES - 1
    for group in range(5):
        found = nn(halo_l[...].astype(BF16), rhs[group])
        for half, target in enumerate(targets(group)):
            for row in range(ext):
                piece = found[row * SUBLANES : (row + 1) * SUBLANES, half * LANES : (half + 1) * LANES]
                target(row)[pl.ds(edge, SUBLANES, stride=SUBLANES), :] = piece

    tile = [pl.ds(SUBLANES * j, SUBLANES) for j in range(chunk)]

    def advance(step, h, first):
        cf = cfs[h].at[pl.ds(first, ROWS)]
        u = us[h].at[pl.ds(first, ROWS + 1)]
        cells = [kept.at[h]] + [u.at[k] for k in range(ROWS + 1)]

        def column(j):
            return [ref[tile[j], :] for ref in cells]

        column_now = column(0)
        last = [ref[tile[chunk - 1], :] for ref in cells[1:-1]]
        wrap = [column_now[k + 1] - pltpu.roll(last[k], 1, 0) for k in range(ROWS)]
        south = wrap
        for j in range(chunk):
            if j + 1 < chunk:
                column_next = column(j + 1)
                north = [column_next[k + 1] - column_now[k + 1] for k in range(ROWS)]
            else:
                column_next = None
                north = [pltpu.roll(x, SUBLANES - 1, 0) for x in wrap]
            east = [column_now[k + 1] - column_now[k] for k in range(ROWS + 1)]
            for k in range(ROWS):
                c = [cf[k, m, tile[j], :] for m in range(4)]
                new = column_now[k + 1] + (
                    (c[0] * east[k + 1] - c[1] * east[k]) + (c[2] * north[k] - c[3] * south[k])
                )
                if step < 4:
                    u[k, tile[j], :] = new
                    continue
                one = node_w[:, h * LANES : (h + 1) * LANES] * new
                two = one * new
                if h == 0:
                    part[k, 0, tile[j], :] = one
                    part[k, 1, tile[j], :] = two
                else:
                    both[k, 0, tile[j], :] = one + part[k, 0, tile[j], :]
                    both[k, 1, tile[j], :] = two + part[k, 1, tile[j], :]
            kept[h, tile[j], :] = column_now[ROWS]
            column_now, south = column_next, north

    def gather_sums(first):
        masks = [(lane == first + k + m * rows, k, m) for k in range(ROWS) for m in range(2)]
        for j in range(chunk):
            old = acc[tile[j], :]
            for mask, k, m in masks:
                old = jnp.where(mask, jnp.sum(both[k, m, tile[j], :], axis=1, keepdims=True), old)
            acc[tile[j], :] = old

    for step, (start, turns) in {1: (0, quads), 2: (2, quads - 1), 3: (1, quads - 1), 4: (HALO, quads - 2)}.items():
        for h in range(2):
            kept[h] = us[h][max(start - 1, 0)]
        if step == 4:
            both[...] = jnp.zeros_like(both)

        @pl.loop(0, turns)
        def _(turn):
            first = start + ROWS * turn
            if step == 4:
                gather_sums(first - HALO - ROWS)
            for h in range(2):
                advance(step, h, first)

    gather_sums(rows - ROWS)

    for j in range(chunk):
        nat[pl.ds(j, SUBLANES, stride=chunk), :] = acc[tile[j], :]
    mine[...] = jnp.transpose(nat[0:LANES, :])
    swap = remote(8, mine, theirs, (1 - core, gx, gy))
    for copy in copies:
        copy.wait_send()
    swap.wait()
    moments_ref[...] = (mine[...] + theirs[...]) / weight_total


def on_device(mesh, field_modes, node_points, quad_weight, group_of):
    rows, cols = field_modes.shape[2:]
    count, dims = node_points.shape
    modes = dims + 1
    ext = rows + 2 * HALO
    ring = cols + 2 * HALO
    kpad = 40
    tiles = rows * HALO // LANES
    vmem = pl.BlockSpec(memory_space=pltpu.VMEM)
    moments = pl.pallas_call(
        functools.partial(kernel, mesh.shape["gx"], mesh.shape["gy"], rows, dims),
        out_shape=jax.ShapeDtypeStruct((2 * rows, cols), F32),
        in_specs=[pl.BlockSpec(memory_space=pl.ANY)] * 4,
        out_specs=vmem,
        scratch_shapes=[
            pltpu.VMEM((kpad * (rows + SUBLANES), LANES), F32),
            pltpu.VMEM((2, kpad * HALO, LANES), F32),
            pltpu.VMEM((2, kpad * HALO, LANES), F32),
            pltpu.VMEM((2, tiles, kpad, LANES), F32),
            pltpu.VMEM((2, tiles, kpad, LANES), F32),
            pltpu.VMEM((4, SUBLANES, LANES), F32),
            pltpu.VMEM((4, SUBLANES, LANES), F32),
            pltpu.VMEM((2, ROWS * ring, LANES), F32),
            pltpu.VMEM((ROWS * ring, LANES), BF16),
            pltpu.VMEM(((2 * tiles + 1) * LANES, LANES), F32),
            pltpu.VMEM((ext * SUBLANES, LANES), F32),
            pltpu.VMEM((5, LANES, 2 * LANES), F32),
            pltpu.VMEM((5, LANES, 2 * LANES), BF16),
            pltpu.VMEM((SUBLANES, SLOTS), F32),
            pltpu.VMEM((2 * SUBLANES, SLOTS), F32),
            pltpu.VMEM((ext, 4, ring, LANES), F32),
            pltpu.VMEM((ext, 4, ring, LANES), F32),
            pltpu.VMEM((ext + 1, ring, LANES), F32),
            pltpu.VMEM((ext + 1, ring, LANES), F32),
            pltpu.VMEM((2, ring, LANES), F32),
            pltpu.VMEM((ROWS, 2, ring, LANES), F32),
            pltpu.VMEM((ROWS, 2, ring, LANES), F32),
            pltpu.VMEM((ring, LANES), F32),
            pltpu.VMEM((ring, LANES), F32),
            pltpu.VMEM((2 * rows, LANES), F32),
            pltpu.VMEM((2 * rows, LANES), F32),
            pltpu.VMEM((dims, count), F32),
            pltpu.VMEM((count,), F32),
            pltpu.VMEM((count,), jnp.int32),
            pltpu.SemaphoreType.DMA((4,)),
            pltpu.SemaphoreType.DMA((9,)),
            pltpu.SemaphoreType.DMA((9,)),
        ],
        compiler_params=pltpu.CompilerParams(
            collective_id=0, has_side_effects=True, vmem_limit_bytes=62 * 1024 * 1024
        ),
    )(
        field_modes.reshape(4 * modes * rows, cols),
        node_points.T,
        quad_weight,
        group_of,
    )
    mean_field = moments[:rows]
    return mean_field, moments[rows:] - mean_field * mean_field


def solution(mesh):
    return jax.shard_map(
        functools.partial(on_device, mesh),
        mesh=mesh,
        in_specs=(P(None, None, "gx", "gy"), P(), P(), P()),
        out_specs=(P("gx", "gy"), P("gx", "gy")),
        check_vma=False,
    )
```

```python
import functools

import jax
import jax.numpy as jnp
from jax import lax
from jax.experimental import pallas as pl
from jax.experimental.pallas import tpu as pltpu
from jax.sharding import PartitionSpec as P

TIME_STEP = 0.15
HALO = 4
LANES = 128
SUBLANES = 8
SLOTS = 256
ROWS = 4
EARLY = 4
MESH = pl.DeviceIdType.MESH
F32 = jnp.float32
BF16 = jnp.bfloat16


def nn(a, b):
    return lax.dot_general(a, b, (((1,), (0,)), ((), ())), preferred_element_type=F32)


def nt(a, b):
    return lax.dot_general(a, b, (((1,), (1,)), ((), ())), preferred_element_type=F32)


def split2(x):
    hi = x.astype(BF16).astype(F32)
    return hi, x - hi


def split3(x):
    hi = x.astype(BF16).astype(F32)
    rest = x - hi
    mid = rest.astype(BF16).astype(F32)
    return hi, mid, rest - mid


def kernel(
    gx_size, gy_size, rows, dims,
    field_hbm, points_hbm, weight_hbm, group_hbm,
    moments_ref,
    fv, send_rows, recv_rows, send_cols, recv_cols, send_corners, recv_corners,
    lnat, left, cols_t, halo_l, rhs_f, rhs, node_w, csc,
    cf0, cf1, ua, ub, kept, part, both, acc, nat, mine, theirs,
    points_ref, weight_ref, group_ref,
    load_sem, send_sem, recv_sem,
):
    ext = rows + 2 * HALO
    quads = ext // ROWS
    modes = dims + 1
    fields = 4 * modes
    ring = LANES + 2 * HALO
    chunk = ring // SUBLANES
    kpad = 40
    groups = kpad // SUBLANES
    core = lax.axis_index("nodes")
    gx = lax.axis_index("gx")
    gy = lax.axis_index("gy")
    xn, xp = lax.rem(gx + 1, gx_size), lax.rem(gx + gx_size - 1, gx_size)
    yn, yp = lax.rem(gy + 1, gy_size), lax.rem(gy + gy_size - 1, gy_size)
    around = [
        (core, xp, gy), (core, xn, gy), (core, gx, yp), (core, gx, yn),
        (core, xp, yp), (core, xp, yn), (core, xn, yp), (core, xn, yn),
        (1 - core, gx, gy),
    ]

    barrier = pltpu.get_barrier_semaphore()
    for device in around:
        pl.semaphore_signal(barrier, inc=1, device_id=device, device_id_type=MESH)

    apart = fv.shape[0] // kpad

    @pl.loop(0, fields)
    def _(k):
        pltpu.make_async_copy(
            field_hbm.at[pl.ds(k * rows, rows)], fv.at[pl.ds(k * apart, rows)], load_sem.at[0]
        ).start()

    small = [
        pltpu.make_async_copy(source, target, load_sem.at[1 + i])
        for i, (source, target) in enumerate(
            [(points_hbm, points_ref), (weight_hbm, weight_ref), (group_hbm, group_ref)]
        )
    ]
    for copy in small:
        copy.start()
    fv[pl.ds(fields * apart, (kpad - fields) * apart), :] = jnp.zeros(((kpad - fields) * apart, LANES), F32)

    for copy in small:
        copy.wait()
    count = group_ref.shape[0]
    included = (group_ref[...].reshape(1, count) < 2).astype(F32)
    weights = weight_ref[...].reshape(1, count)
    weight_total = jnp.sum(weights * included, axis=1, keepdims=True)
    row8 = lax.broadcasted_iota(jnp.int32, (SUBLANES, LANES), 0)
    blocks = count // LANES
    pieces = [included[:, b * LANES : (b + 1) * LANES] for b in range(blocks)]
    stacked = jnp.zeros((SUBLANES, LANES), F32)
    for b in range(blocks):
        stacked = jnp.where(row8 == b, jnp.broadcast_to(pieces[b], (SUBLANES, LANES)), stacked)
    before = lax.broadcasted_iota(jnp.int32, (LANES, LANES), 0) <= lax.broadcasted_iota(jnp.int32, (LANES, LANES), 1)
    within = nn(stacked.astype(BF16), before.astype(F32).astype(BF16))
    totals = jnp.sum(stacked, axis=1, keepdims=True)
    slot = (lax.broadcasted_iota(jnp.int32, (SLOTS, LANES), 0) + (core * SLOTS + 1)).astype(F32)
    offset = jnp.zeros((1, 1), F32)
    chosen = []
    for b in range(blocks):
        order = within[b : b + 1] + offset
        offset = offset + totals[b : b + 1]
        order = jnp.where(pieces[b] > 0, order, 0.0)
        chosen.append(jnp.where(slot == jnp.broadcast_to(order, (SLOTS, LANES)), 1.0, 0.0).astype(BF16))
    select = jnp.concatenate(chosen, axis=1)
    w_hi, w_mid, w_lo = split3(weights)
    w_rows = lax.broadcasted_iota(jnp.int32, (SUBLANES, count), 0)
    w_stack = jnp.where(w_rows == 0, w_hi, jnp.where(w_rows == 1, w_mid, jnp.where(w_rows == 2, w_lo, 0.0)))
    found = nt(jnp.concatenate([*split3(points_ref[...]), w_stack], axis=0).astype(BF16), select)
    coords = found[0:dims] + found[dims : 2 * dims] + found[2 * dims : 3 * dims]
    held = found[3 * dims : 3 * dims + 1] + found[3 * dims + 1 : 3 * dims + 2] + found[3 * dims + 2 : 3 * dims + 3]
    node_w[...] = jnp.broadcast_to(held, (SUBLANES, SLOTS))

    csc[0:1, :] = jnp.ones((1, SLOTS), F32)
    csc[1 : 1 + dims, :] = coords
    coefficient = csc[...][0:modes]
    rhs_f[...] = jnp.zeros_like(rhs_f)

    def place(group, half, h, field, scale):
        hi, lo = split2(coefficient[:, h * LANES : (h + 1) * LANES] * scale)
        at = field * modes
        lanes = pl.ds(half * LANES, LANES)
        rhs_f[group, pl.ds(at, modes), lanes] = hi
        rhs_f[group, pl.ds(kpad + at, modes), lanes] = lo
        rhs_f[group, pl.ds(2 * kpad + at, modes), lanes] = hi

    for h in range(2):
        for k in range(4):
            place(2 * h + k // 2, k % 2, h, 3, TIME_STEP)
            place(2 * h + k // 2, k % 2, h, 1 + k // 2, (-0.5, 0.5)[k % 2] * TIME_STEP)
        place(4, h, h, 0, 1.0)
    rhs[...] = rhs_f[...].astype(BF16)

    rest = jnp.zeros((SUBLANES, LANES), F32)

    def turned(x):
        hi, lo = split2(x)
        stack = jnp.concatenate([hi, hi, lo, rest], axis=0).astype(BF16)
        return jnp.transpose(stack).astype(F32)

    def turn_rows(quad):
        for k in range(ROWS):
            x = fv[pl.ds(ROWS * quad - HALO + k, kpad, stride=apart), :]
            lnat[lax.rem(quad, 2), pl.ds(k * ring, LANES), :] = turned(x)

    cfs, us = (cf0, cf1), (ua, ub)

    def targets(group):
        if group == 4:
            return [lambda row: us[0].at[row], lambda row: us[1].at[row]]
        return [
            lambda row: cfs[group // 2].at[row, 2 * (group % 2)],
            lambda row: cfs[group // 2].at[row, 2 * (group % 2) + 1],
        ]

    def parameters(quad):
        slot = lax.rem(quad, 2)
        cells = []
        for k in range(ROWS):
            cells += [lnat[slot, pl.ds(k * ring + j, SUBLANES, stride=chunk), :] for j in range(chunk)]
        left[...] = jnp.concatenate(cells, axis=0).astype(BF16)
        for group in range(5):
            found = nn(left[...], rhs[group])
            for half, target in enumerate(targets(group)):
                for k in range(ROWS):
                    piece = found[k * ring : (k + 1) * ring, half * LANES : (half + 1) * LANES]
                    target(ROWS * quad + k)[...] = piece

    sent = fields * HALO
    for side in range(2):
        recv_rows[side, pl.ds(sent, kpad * HALO - sent), :] = jnp.zeros((kpad * HALO - sent, LANES), F32)
    acc[...] = jnp.zeros_like(acc)
    pltpu.make_async_copy(field_hbm, fv.at[pl.ds(0, fields * rows)], load_sem.at[0]).wait()

    lane = lax.broadcasted_iota(jnp.int32, (SUBLANES, LANES), 1)
    by_halo = lane // HALO
    block = HALO * HALO
    by_block = lane // block
    per_tile = LANES // HALO
    tiles = rows // per_tile

    for r in range(HALO):
        send_rows[0, pl.ds(r, kpad, stride=HALO), :] = fv[pl.ds(r, kpad, stride=apart), :]
        send_rows[1, pl.ds(r, kpad, stride=HALO), :] = fv[pl.ds(rows - HALO + r, kpad, stride=apart), :]
    for t in range(tiles):
        low = [jnp.zeros((SUBLANES, LANES), F32)] * groups
        high = [jnp.zeros((SUBLANES, LANES), F32)] * groups
        for g in range(per_tile):
            at_high = by_halo == g
            at_low = by_halo == (g + 1) % per_tile
            for m in range(groups):
                x = fv[pl.ds(m * SUBLANES * apart + t * per_tile + g, SUBLANES, stride=apart), :]
                x = pltpu.roll(x, (HALO * (g + 1)) % LANES, 1)
                high[m] = jnp.where(at_high, x, high[m])
                low[m] = jnp.where(at_low, x, low[m])
        for side, values in enumerate((low, high)):
            for m in range(groups):
                send_cols[side, t, m * SUBLANES : (m + 1) * SUBLANES, :] = values[m]
            for end in range(2):
                if t != (0, tiles - 1)[end]:
                    continue
                at = HALO * (1 - side) + (0, LANES - block)[end]
                packed = jnp.zeros((SUBLANES, LANES), F32)
                for m in range(groups):
                    packed = jnp.where(by_block == m, pltpu.roll(values[m], (block * m - at) % LANES, 1), packed)
                send_corners[2 * end + side] = packed

    turn_rows(1)

    @pl.loop(1, 1 + EARLY)
    def _(quad):
        parameters(quad)
        turn_rows(quad + 1)

    pl.semaphore_wait(barrier, len(around))

    def remote(index, source, target, device):
        copy = pltpu.make_async_remote_copy(
            src_ref=source, dst_ref=target,
            send_sem=send_sem.at[index], recv_sem=recv_sem.at[index],
            device_id=device, device_id_type=MESH,
        )
        copy.start()
        return copy

    copies = [
        remote(0, send_rows.at[0, pl.ds(0, sent)], recv_rows.at[0, pl.ds(0, sent)], (core, xp, gy)),
        remote(1, send_rows.at[1, pl.ds(0, sent)], recv_rows.at[1, pl.ds(0, sent)], (core, xn, gy)),
        remote(2, send_cols.at[0], recv_cols.at[0], (core, gx, yp)),
        remote(3, send_cols.at[1], recv_cols.at[1], (core, gx, yn)),
        remote(4, send_corners.at[0], recv_corners.at[0], (core, xp, yp)),
        remote(5, send_corners.at[1], recv_corners.at[1], (core, xp, yn)),
        remote(6, send_corners.at[2], recv_corners.at[2], (core, xn, yp)),
        remote(7, send_corners.at[3], recv_corners.at[3], (core, xn, yn)),
    ]

    @pl.loop(1 + EARLY, quads - 2)
    def _(quad):
        parameters(quad)
        turn_rows(quad + 1)

    parameters(quads - 2)

    for copy in copies:
        copy.wait_recv()

    for side, quad in ((1, 0), (0, quads - 1)):
        for k in range(ROWS):
            x = recv_rows[side, pl.ds(k, kpad, stride=HALO), :]
            lnat[quad % 2, pl.ds(k * ring, LANES), :] = turned(x)
        parameters(quad)

    for t in range(2 * tiles):
        cols_t[pl.ds(t * LANES, LANES), :] = turned(recv_cols[t // tiles, t % tiles])
    corners = [recv_corners[k] for k in range(4)]
    unpacked = []
    for m in range(groups):
        x = jnp.zeros((SUBLANES, LANES), F32)
        for k in range(4):
            x = jnp.where(by_block == k, pltpu.roll(corners[k], block * (k - m) % LANES, 1), x)
        unpacked.append(x)
    cols_t[pl.ds(2 * tiles * LANES, LANES), :] = turned(jnp.concatenate(unpacked, axis=0))

    def column_halo(row, right, left_side):
        halo_l[pl.ds(row * SUBLANES, HALO), :] = cols_t[pl.ds(right, HALO), :]
        halo_l[pl.ds(row * SUBLANES + HALO, HALO), :] = cols_t[pl.ds(left_side, HALO), :]

    for row in range(rows):
        t, g = divmod(row, per_tile)
        column_halo(
            row + HALO,
            t * LANES + HALO * ((g + 1) % per_tile),
            (tiles + t) * LANES + HALO * g,
        )
    corner = 2 * tiles * LANES
    for r in range(HALO):
        column_halo(rows + HALO + r, corner + HALO * r, corner + block + HALO * r)
        column_halo(r, corner + 2 * block + HALO * r, corner + 3 * block + HALO * r)
    edge = (chunk - SUBLANES) * SUBLANES + SUBLANES - 1
    for group in range(5):
        found = nn(halo_l[...].astype(BF16), rhs[group])
        for half, target in enumerate(targets(group)):
            for row in range(ext):
                piece = found[row * SUBLANES : (row + 1) * SUBLANES, half * LANES : (half + 1) * LANES]
                target(row)[pl.ds(edge, SUBLANES, stride=SUBLANES), :] = piece

    tile = [pl.ds(SUBLANES * j, SUBLANES) for j in range(chunk)]

    def advance(step, h, first):
        cf = cfs[h].at[pl.ds(first, ROWS)]
        u = us[h].at[pl.ds(first, ROWS + 1)]
        cells = [kept.at[h]] + [u.at[k] for k in range(ROWS + 1)]

        def column(j):
            return [ref[tile[j], :] for ref in cells]

        column_now = column(0)
        last = [ref[tile[chunk - 1], :] for ref in cells[1:-1]]
        wrap = [column_now[k + 1] - pltpu.roll(last[k], 1, 0) for k in range(ROWS)]
        south = wrap
        for j in range(chunk):
            if j + 1 < chunk:
                column_next = column(j + 1)
                north = [column_next[k + 1] - column_now[k + 1] for k in range(ROWS)]
            else:
                column_next = None
                north = [pltpu.roll(x, SUBLANES - 1, 0) for x in wrap]
            east = [column_now[k + 1] - column_now[k] for k in range(ROWS + 1)]
            for k in range(ROWS):
                c = [cf[k, m, tile[j], :] for m in range(4)]
                new = column_now[k + 1] + (
                    (c[0] * east[k + 1] - c[1] * east[k]) + (c[2] * north[k] - c[3] * south[k])
                )
                if step < 4:
                    u[k, tile[j], :] = new
                    continue
                one = node_w[:, h * LANES : (h + 1) * LANES] * new
                two = one * new
                if h == 0:
                    part[k, 0, tile[j], :] = one
                    part[k, 1, tile[j], :] = two
                else:
                    both[k, 0, tile[j], :] = one + part[k, 0, tile[j], :]
                    both[k, 1, tile[j], :] = two + part[k, 1, tile[j], :]
            kept[h, tile[j], :] = column_now[ROWS]
            column_now, south = column_next, north

    def gather_sums(first):
        masks = [(lane == first + k + m * rows, k, m) for k in range(ROWS) for m in range(2)]
        for j in range(chunk):
            old = acc[tile[j], :]
            for mask, k, m in masks:
                old = jnp.where(mask, jnp.sum(both[k, m, tile[j], :], axis=1, keepdims=True), old)
            acc[tile[j], :] = old

    for step, (start, turns) in {1: (0, quads), 2: (2, quads - 1), 3: (1, quads - 1), 4: (HALO, quads - 2)}.items():
        for h in range(2):
            kept[h] = us[h][max(start - 1, 0)]
        if step == 4:
            both[...] = jnp.zeros_like(both)

        @pl.loop(0, turns)
        def _(turn):
            first = start + ROWS * turn
            if step == 4:
                gather_sums(first - HALO - ROWS)
            for h in range(2):
                advance(step, h, first)

    gather_sums(rows - ROWS)

    for j in range(chunk):
        nat[pl.ds(j, SUBLANES, stride=chunk), :] = acc[tile[j], :]
    mine[...] = jnp.transpose(nat[0:LANES, :])
    swap = remote(8, mine, theirs, (1 - core, gx, gy))
    for copy in copies:
        copy.wait_send()
    swap.wait()
    moments_ref[...] = (mine[...] + theirs[...]) / weight_total


def on_device(mesh, field_modes, node_points, quad_weight, group_of):
    rows, cols = field_modes.shape[2:]
    count, dims = node_points.shape
    modes = dims + 1
    ext = rows + 2 * HALO
    ring = cols + 2 * HALO
    kpad = 40
    tiles = rows * HALO // LANES
    vmem = pl.BlockSpec(memory_space=pltpu.VMEM)
    moments = pl.pallas_call(
        functools.partial(kernel, mesh.shape["gx"], mesh.shape["gy"], rows, dims),
        out_shape=pltpu.VMEM((2 * rows, cols), F32),
        in_specs=[pl.BlockSpec(memory_space=pl.ANY)] * 4,
        out_specs=vmem,
        scratch_shapes=[
            pltpu.VMEM((kpad * (rows + SUBLANES), LANES), F32),
            pltpu.VMEM((2, kpad * HALO, LANES), F32),
            pltpu.VMEM((2, kpad * HALO, LANES), F32),
            pltpu.VMEM((2, tiles, kpad, LANES), F32),
            pltpu.VMEM((2, tiles, kpad, LANES), F32),
            pltpu.VMEM((4, SUBLANES, LANES), F32),
            pltpu.VMEM((4, SUBLANES, LANES), F32),
            pltpu.VMEM((2, ROWS * ring, LANES), F32),
            pltpu.VMEM((ROWS * ring, LANES), BF16),
            pltpu.VMEM(((2 * tiles + 1) * LANES, LANES), F32),
            pltpu.VMEM((ext * SUBLANES, LANES), F32),
            pltpu.VMEM((5, LANES, 2 * LANES), F32),
            pltpu.VMEM((5, LANES, 2 * LANES), BF16),
            pltpu.VMEM((SUBLANES, SLOTS), F32),
            pltpu.VMEM((2 * SUBLANES, SLOTS), F32),
            pltpu.VMEM((ext, 4, ring, LANES), F32),
            pltpu.VMEM((ext, 4, ring, LANES), F32),
            pltpu.VMEM((ext + 1, ring, LANES), F32),
            pltpu.VMEM((ext + 1, ring, LANES), F32),
            pltpu.VMEM((2, ring, LANES), F32),
            pltpu.VMEM((ROWS, 2, ring, LANES), F32),
            pltpu.VMEM((ROWS, 2, ring, LANES), F32),
            pltpu.VMEM((ring, LANES), F32),
            pltpu.VMEM((ring, LANES), F32),
            pltpu.VMEM((2 * rows, LANES), F32),
            pltpu.VMEM((2 * rows, LANES), F32),
            pltpu.VMEM((dims, count), F32),
            pltpu.VMEM((count,), F32),
            pltpu.VMEM((count,), jnp.int32),
            pltpu.SemaphoreType.DMA((4,)),
            pltpu.SemaphoreType.DMA((9,)),
            pltpu.SemaphoreType.DMA((9,)),
        ],
        compiler_params=pltpu.CompilerParams(
            collective_id=0, has_side_effects=True, vmem_limit_bytes=62 * 1024 * 1024
        ),
    )(
        field_modes.reshape(4 * modes * rows, cols),
        node_points.T,
        quad_weight,
        group_of,
    )
    mean_field = moments[:rows]
    return mean_field, moments[rows:] - mean_field * mean_field


def solution(mesh):
    return jax.shard_map(
        functools.partial(on_device, mesh),
        mesh=mesh,
        in_specs=(P(None, None, "gx", "gy"), P(), P(), P()),
        out_specs=(P("gx", "gy"), P("gx", "gy")),
        check_vma=False,
    )
```

```python
import functools

import jax
import jax.numpy as jnp
from jax import lax
from jax.experimental import pallas as pl
from jax.experimental.pallas import tpu as pltpu
from jax.sharding import PartitionSpec as P

TIME_STEP = 0.15
HALO = 4
LANES = 128
SUBLANES = 8
SLOTS = 256
ROWS = 4
EARLY = 4
MESH = pl.DeviceIdType.MESH
F32 = jnp.float32
BF16 = jnp.bfloat16


def nn(a, b):
    return lax.dot_general(a, b, (((1,), (0,)), ((), ())), preferred_element_type=F32)


def nt(a, b):
    return lax.dot_general(a, b, (((1,), (1,)), ((), ())), preferred_element_type=F32)


def split2(x):
    hi = x.astype(BF16).astype(F32)
    return hi, x - hi


def split3(x):
    hi = x.astype(BF16).astype(F32)
    rest = x - hi
    mid = rest.astype(BF16).astype(F32)
    return hi, mid, rest - mid


def kernel(
    gx_size, gy_size, rows, dims,
    field_hbm, points_hbm, weight_hbm, group_hbm,
    moments_ref,
    fv, send_rows, recv_rows, send_cols, recv_cols, send_corners, recv_corners,
    lnat, left, cols_t, halo_l, rhs_f, rhs, node_w, csc,
    cf0, cf1, ua, ub, kept, part, both, acc, nat, mine, theirs,
    points_ref, weight_ref, group_ref,
    load_sem, send_sem, recv_sem,
):
    ext = rows + 2 * HALO
    quads = ext // ROWS
    modes = dims + 1
    fields = 4 * modes
    ring = LANES + 2 * HALO
    chunk = ring // SUBLANES
    kpad = 40
    groups = kpad // SUBLANES
    core = lax.axis_index("nodes")
    gx = lax.axis_index("gx")
    gy = lax.axis_index("gy")
    xn, xp = lax.rem(gx + 1, gx_size), lax.rem(gx + gx_size - 1, gx_size)
    yn, yp = lax.rem(gy + 1, gy_size), lax.rem(gy + gy_size - 1, gy_size)
    around = [
        (core, xp, gy), (core, xn, gy), (core, gx, yp), (core, gx, yn),
        (core, xp, yp), (core, xp, yn), (core, xn, yp), (core, xn, yn),
        (1 - core, gx, gy),
    ]

    barrier = pltpu.get_barrier_semaphore()
    for device in around:
        pl.semaphore_signal(barrier, inc=1, device_id=device, device_id_type=MESH)

    apart = fv.shape[0] // kpad

    @pl.loop(0, fields)
    def _(k):
        pltpu.make_async_copy(
            field_hbm.at[pl.ds(k * rows, rows)], fv.at[pl.ds(k * apart, rows)], load_sem.at[0]
        ).start()

    small = [
        pltpu.make_async_copy(source, target, load_sem.at[1 + i])
        for i, (source, target) in enumerate(
            [(points_hbm, points_ref), (weight_hbm, weight_ref), (group_hbm, group_ref)]
        )
    ]
    for copy in small:
        copy.start()
    fv[pl.ds(fields * apart, (kpad - fields) * apart), :] = jnp.zeros(((kpad - fields) * apart, LANES), F32)

    for copy in small:
        copy.wait()
    count = group_ref.shape[0]
    included = (group_ref[...].reshape(1, count) < 2).astype(F32)
    weights = weight_ref[...].reshape(1, count)
    weight_total = jnp.sum(weights * included, axis=1, keepdims=True)
    row8 = lax.broadcasted_iota(jnp.int32, (SUBLANES, LANES), 0)
    blocks = count // LANES
    pieces = [included[:, b * LANES : (b + 1) * LANES] for b in range(blocks)]
    stacked = jnp.zeros((SUBLANES, LANES), F32)
    for b in range(blocks):
        stacked = jnp.where(row8 == b, jnp.broadcast_to(pieces[b], (SUBLANES, LANES)), stacked)
    before = lax.broadcasted_iota(jnp.int32, (LANES, LANES), 0) <= lax.broadcasted_iota(jnp.int32, (LANES, LANES), 1)
    within = nn(stacked.astype(BF16), before.astype(F32).astype(BF16))
    totals = jnp.sum(stacked, axis=1, keepdims=True)
    slot = (lax.broadcasted_iota(jnp.int32, (SLOTS, LANES), 0) + (core * SLOTS + 1)).astype(F32)
    offset = jnp.zeros((1, 1), F32)
    chosen = []
    for b in range(blocks):
        order = within[b : b + 1] + offset
        offset = offset + totals[b : b + 1]
        order = jnp.where(pieces[b] > 0, order, 0.0)
        chosen.append(jnp.where(slot == jnp.broadcast_to(order, (SLOTS, LANES)), 1.0, 0.0).astype(BF16))
    select = jnp.concatenate(chosen, axis=1)
    w_hi, w_mid, w_lo = split3(weights)
    w_rows = lax.broadcasted_iota(jnp.int32, (SUBLANES, count), 0)
    w_stack = jnp.where(w_rows == 0, w_hi, jnp.where(w_rows == 1, w_mid, jnp.where(w_rows == 2, w_lo, 0.0)))
    found = nt(jnp.concatenate([*split3(points_ref[...]), w_stack], axis=0).astype(BF16), select)
    coords = found[0:dims] + found[dims : 2 * dims] + found[2 * dims : 3 * dims]
    held = found[3 * dims : 3 * dims + 1] + found[3 * dims + 1 : 3 * dims + 2] + found[3 * dims + 2 : 3 * dims + 3]
    node_w[...] = jnp.broadcast_to(held, (SUBLANES, SLOTS))

    csc[0:1, :] = jnp.ones((1, SLOTS), F32)
    csc[1 : 1 + dims, :] = coords
    coefficient = csc[...][0:modes]
    rhs_f[...] = jnp.zeros_like(rhs_f)

    def place(group, half, h, field, scale):
        hi, lo = split2(coefficient[:, h * LANES : (h + 1) * LANES] * scale)
        at = field * modes
        lanes = pl.ds(half * LANES, LANES)
        rhs_f[group, pl.ds(at, modes), lanes] = hi
        rhs_f[group, pl.ds(kpad + at, modes), lanes] = lo
        rhs_f[group, pl.ds(2 * kpad + at, modes), lanes] = hi

    for h in range(2):
        for k in range(4):
            place(2 * h + k // 2, k % 2, h, 3, TIME_STEP)
            place(2 * h + k // 2, k % 2, h, 1 + k // 2, (-0.5, 0.5)[k % 2] * TIME_STEP)
        place(4, h, h, 0, 1.0)
    rhs[...] = rhs_f[...].astype(BF16)

    rest = jnp.zeros((SUBLANES, LANES), F32)

    def turned(x):
        hi, lo = split2(x)
        stack = jnp.concatenate([hi, hi, lo, rest], axis=0).astype(BF16)
        return jnp.transpose(stack).astype(F32)

    def turn_rows(quad):
        for k in range(ROWS):
            x = fv[pl.ds(ROWS * quad - HALO + k, kpad, stride=apart), :]
            lnat[lax.rem(quad, 2), pl.ds(k * ring, LANES), :] = turned(x)

    cfs, us = (cf0, cf1), (ua, ub)

    def targets(group):
        if group == 4:
            return [lambda row: us[0].at[row], lambda row: us[1].at[row]]
        return [
            lambda row: cfs[group // 2].at[row, 2 * (group % 2)],
            lambda row: cfs[group // 2].at[row, 2 * (group % 2) + 1],
        ]

    def parameters(quad):
        slot = lax.rem(quad, 2)
        cells = []
        for k in range(ROWS):
            cells += [lnat[slot, pl.ds(k * ring + j, SUBLANES, stride=chunk), :] for j in range(chunk)]
        left[...] = jnp.concatenate(cells, axis=0).astype(BF16)
        for group in range(5):
            found = nn(left[...], rhs[group])
            for half, target in enumerate(targets(group)):
                for k in range(ROWS):
                    piece = found[k * ring : (k + 1) * ring, half * LANES : (half + 1) * LANES]
                    target(ROWS * quad + k)[...] = piece

    sent = fields * HALO
    for side in range(2):
        recv_rows[side, pl.ds(sent, kpad * HALO - sent), :] = jnp.zeros((kpad * HALO - sent, LANES), F32)
    acc[...] = jnp.zeros_like(acc)
    pltpu.make_async_copy(field_hbm, fv.at[pl.ds(0, fields * rows)], load_sem.at[0]).wait()

    lane = lax.broadcasted_iota(jnp.int32, (SUBLANES, LANES), 1)
    by_halo = lane // HALO
    block = HALO * HALO
    by_block = lane // block
    per_tile = LANES // HALO
    tiles = rows // per_tile

    for r in range(HALO):
        send_rows[0, pl.ds(r, kpad, stride=HALO), :] = fv[pl.ds(r, kpad, stride=apart), :]
        send_rows[1, pl.ds(r, kpad, stride=HALO), :] = fv[pl.ds(rows - HALO + r, kpad, stride=apart), :]
    for t in range(tiles):
        low = [jnp.zeros((SUBLANES, LANES), F32)] * groups
        high = [jnp.zeros((SUBLANES, LANES), F32)] * groups
        for g in range(per_tile):
            at_high = by_halo == g
            at_low = by_halo == (g + 1) % per_tile
            for m in range(groups):
                x = fv[pl.ds(m * SUBLANES * apart + t * per_tile + g, SUBLANES, stride=apart), :]
                x = pltpu.roll(x, (HALO * (g + 1)) % LANES, 1)
                high[m] = jnp.where(at_high, x, high[m])
                low[m] = jnp.where(at_low, x, low[m])
        for side, values in enumerate((low, high)):
            for m in range(groups):
                send_cols[side, t, m * SUBLANES : (m + 1) * SUBLANES, :] = values[m]
            for end in range(2):
                if t != (0, tiles - 1)[end]:
                    continue
                at = HALO * (1 - side) + (0, LANES - block)[end]
                packed = jnp.zeros((SUBLANES, LANES), F32)
                for m in range(groups):
                    packed = jnp.where(by_block == m, pltpu.roll(values[m], (block * m - at) % LANES, 1), packed)
                send_corners[2 * end + side] = packed

    turn_rows(1)

    @pl.loop(1, 1 + EARLY)
    def _(quad):
        parameters(quad)
        turn_rows(quad + 1)

    pl.semaphore_wait(barrier, len(around))

    def remote(index, source, target, device):
        copy = pltpu.make_async_remote_copy(
            src_ref=source, dst_ref=target,
            send_sem=send_sem.at[index], recv_sem=recv_sem.at[index],
            device_id=device, device_id_type=MESH,
        )
        copy.start()
        return copy

    copies = [
        remote(4, send_corners.at[0], recv_corners.at[0], (core, xp, yp)),
        remote(5, send_corners.at[1], recv_corners.at[1], (core, xp, yn)),
        remote(6, send_corners.at[2], recv_corners.at[2], (core, xn, yp)),
        remote(7, send_corners.at[3], recv_corners.at[3], (core, xn, yn)),
        remote(0, send_rows.at[0, pl.ds(0, sent)], recv_rows.at[0, pl.ds(0, sent)], (core, xp, gy)),
        remote(1, send_rows.at[1, pl.ds(0, sent)], recv_rows.at[1, pl.ds(0, sent)], (core, xn, gy)),
        remote(2, send_cols.at[0], recv_cols.at[0], (core, gx, yp)),
        remote(3, send_cols.at[1], recv_cols.at[1], (core, gx, yn)),
    ]

    @pl.loop(1 + EARLY, quads - 2)
    def _(quad):
        parameters(quad)
        turn_rows(quad + 1)

    parameters(quads - 2)

    for copy in copies:
        copy.wait_recv()

    for side, quad in ((1, 0), (0, quads - 1)):
        for k in range(ROWS):
            x = recv_rows[side, pl.ds(k, kpad, stride=HALO), :]
            lnat[quad % 2, pl.ds(k * ring, LANES), :] = turned(x)
        parameters(quad)

    for t in range(2 * tiles):
        cols_t[pl.ds(t * LANES, LANES), :] = turned(recv_cols[t // tiles, t % tiles])
    corners = [recv_corners[k] for k in range(4)]
    unpacked = []
    for m in range(groups):
        x = jnp.zeros((SUBLANES, LANES), F32)
        for k in range(4):
            x = jnp.where(by_block == k, pltpu.roll(corners[k], block * (k - m) % LANES, 1), x)
        unpacked.append(x)
    cols_t[pl.ds(2 * tiles * LANES, LANES), :] = turned(jnp.concatenate(unpacked, axis=0))

    def column_halo(row, right, left_side):
        halo_l[pl.ds(row * SUBLANES, HALO), :] = cols_t[pl.ds(right, HALO), :]
        halo_l[pl.ds(row * SUBLANES + HALO, HALO), :] = cols_t[pl.ds(left_side, HALO), :]

    for row in range(rows):
        t, g = divmod(row, per_tile)
        column_halo(
            row + HALO,
            t * LANES + HALO * ((g + 1) % per_tile),
            (tiles + t) * LANES + HALO * g,
        )
    corner = 2 * tiles * LANES
    for r in range(HALO):
        column_halo(rows + HALO + r, corner + HALO * r, corner + block + HALO * r)
        column_halo(r, corner + 2 * block + HALO * r, corner + 3 * block + HALO * r)
    edge = (chunk - SUBLANES) * SUBLANES + SUBLANES - 1
    for group in range(5):
        found = nn(halo_l[...].astype(BF16), rhs[group])
        for half, target in enumerate(targets(group)):
            for row in range(ext):
                piece = found[row * SUBLANES : (row + 1) * SUBLANES, half * LANES : (half + 1) * LANES]
                target(row)[pl.ds(edge, SUBLANES, stride=SUBLANES), :] = piece

    tile = [pl.ds(SUBLANES * j, SUBLANES) for j in range(chunk)]

    def advance(step, h, first):
        cf = cfs[h].at[pl.ds(first, ROWS)]
        u = us[h].at[pl.ds(first, ROWS + 1)]
        cells = [kept.at[h]] + [u.at[k] for k in range(ROWS + 1)]

        def column(j):
            return [ref[tile[j], :] for ref in cells]

        column_now = column(0)
        last = [ref[tile[chunk - 1], :] for ref in cells[1:-1]]
        wrap = [column_now[k + 1] - pltpu.roll(last[k], 1, 0) for k in range(ROWS)]
        south = wrap
        for j in range(chunk):
            if j + 1 < chunk:
                column_next = column(j + 1)
                north = [column_next[k + 1] - column_now[k + 1] for k in range(ROWS)]
            else:
                column_next = None
                north = [pltpu.roll(x, SUBLANES - 1, 0) for x in wrap]
            east = [column_now[k + 1] - column_now[k] for k in range(ROWS + 1)]
            for k in range(ROWS):
                c = [cf[k, m, tile[j], :] for m in range(4)]
                new = column_now[k + 1] + (
                    (c[0] * east[k + 1] - c[1] * east[k]) + (c[2] * north[k] - c[3] * south[k])
                )
                if step < 4:
                    u[k, tile[j], :] = new
                    continue
                one = node_w[:, h * LANES : (h + 1) * LANES] * new
                two = one * new
                if h == 0:
                    part[k, 0, tile[j], :] = one
                    part[k, 1, tile[j], :] = two
                else:
                    both[k, 0, tile[j], :] = one + part[k, 0, tile[j], :]
                    both[k, 1, tile[j], :] = two + part[k, 1, tile[j], :]
            kept[h, tile[j], :] = column_now[ROWS]
            column_now, south = column_next, north

    def gather_sums(first):
        masks = [(lane == first + k + m * rows, k, m) for k in range(ROWS) for m in range(2)]
        for j in range(chunk):
            old = acc[tile[j], :]
            for mask, k, m in masks:
                old = jnp.where(mask, jnp.sum(both[k, m, tile[j], :], axis=1, keepdims=True), old)
            acc[tile[j], :] = old

    for step, (start, turns) in {1: (0, quads), 2: (2, quads - 1), 3: (1, quads - 1), 4: (HALO, quads - 2)}.items():
        for h in range(2):
            kept[h] = us[h][max(start - 1, 0)]
        if step == 4:
            both[...] = jnp.zeros_like(both)

        @pl.loop(0, turns)
        def _(turn):
            first = start + ROWS * turn
            if step == 4:
                gather_sums(first - HALO - ROWS)
            for h in range(2):
                advance(step, h, first)

    gather_sums(rows - ROWS)

    for j in range(chunk):
        nat[pl.ds(j, SUBLANES, stride=chunk), :] = acc[tile[j], :]
    mine[...] = jnp.transpose(nat[0:LANES, :])
    swap = remote(8, mine, theirs, (1 - core, gx, gy))
    for copy in copies:
        copy.wait_send()
    swap.wait()
    moments_ref[...] = (mine[...] + theirs[...]) / weight_total


def on_device(mesh, field_modes, node_points, quad_weight, group_of):
    rows, cols = field_modes.shape[2:]
    count, dims = node_points.shape
    modes = dims + 1
    ext = rows + 2 * HALO
    ring = cols + 2 * HALO
    kpad = 40
    tiles = rows * HALO // LANES
    vmem = pl.BlockSpec(memory_space=pltpu.VMEM)
    moments = pl.pallas_call(
        functools.partial(kernel, mesh.shape["gx"], mesh.shape["gy"], rows, dims),
        out_shape=pltpu.VMEM((2 * rows, cols), F32),
        in_specs=[pl.BlockSpec(memory_space=pl.ANY)] * 4,
        out_specs=vmem,
        scratch_shapes=[
            pltpu.VMEM((kpad * (rows + SUBLANES), LANES), F32),
            pltpu.VMEM((2, kpad * HALO, LANES), F32),
            pltpu.VMEM((2, kpad * HALO, LANES), F32),
            pltpu.VMEM((2, tiles, kpad, LANES), F32),
            pltpu.VMEM((2, tiles, kpad, LANES), F32),
            pltpu.VMEM((4, SUBLANES, LANES), F32),
            pltpu.VMEM((4, SUBLANES, LANES), F32),
            pltpu.VMEM((2, ROWS * ring, LANES), F32),
            pltpu.VMEM((ROWS * ring, LANES), BF16),
            pltpu.VMEM(((2 * tiles + 1) * LANES, LANES), F32),
            pltpu.VMEM((ext * SUBLANES, LANES), F32),
            pltpu.VMEM((5, LANES, 2 * LANES), F32),
            pltpu.VMEM((5, LANES, 2 * LANES), BF16),
            pltpu.VMEM((SUBLANES, SLOTS), F32),
            pltpu.VMEM((2 * SUBLANES, SLOTS), F32),
            pltpu.VMEM((ext, 4, ring, LANES), F32),
            pltpu.VMEM((ext, 4, ring, LANES), F32),
            pltpu.VMEM((ext + 1, ring, LANES), F32),
            pltpu.VMEM((ext + 1, ring, LANES), F32),
            pltpu.VMEM((2, ring, LANES), F32),
            pltpu.VMEM((ROWS, 2, ring, LANES), F32),
            pltpu.VMEM((ROWS, 2, ring, LANES), F32),
            pltpu.VMEM((ring, LANES), F32),
            pltpu.VMEM((ring, LANES), F32),
            pltpu.VMEM((2 * rows, LANES), F32),
            pltpu.VMEM((2 * rows, LANES), F32),
            pltpu.VMEM((dims, count), F32),
            pltpu.VMEM((count,), F32),
            pltpu.VMEM((count,), jnp.int32),
            pltpu.SemaphoreType.DMA((4,)),
            pltpu.SemaphoreType.DMA((9,)),
            pltpu.SemaphoreType.DMA((9,)),
        ],
        compiler_params=pltpu.CompilerParams(
            collective_id=0, has_side_effects=True, vmem_limit_bytes=62 * 1024 * 1024
        ),
    )(
        field_modes.reshape(4 * modes * rows, cols),
        node_points.T,
        quad_weight,
        group_of,
    )
    mean_field = moments[:rows]
    return mean_field, moments[rows:] - mean_field * mean_field


def solution(mesh):
    return jax.shard_map(
        functools.partial(on_device, mesh),
        mesh=mesh,
        in_specs=(P(None, None, "gx", "gy"), P(), P(), P()),
        out_specs=(P("gx", "gy"), P("gx", "gy")),
        check_vma=False,
    )
```

```python
import functools

import jax
import jax.numpy as jnp
from jax import lax
from jax.experimental import pallas as pl
from jax.experimental.pallas import tpu as pltpu
from jax.sharding import PartitionSpec as P

TIME_STEP = 0.15
HALO = 4
LANES = 128
SUBLANES = 8
SLOTS = 256
ROWS = 4
EARLY = 4
MESH = pl.DeviceIdType.MESH
F32 = jnp.float32
BF16 = jnp.bfloat16


def nn(a, b):
    return lax.dot_general(a, b, (((1,), (0,)), ((), ())), preferred_element_type=F32)


def nt(a, b):
    return lax.dot_general(a, b, (((1,), (1,)), ((), ())), preferred_element_type=F32)


def split2(x):
    hi = x.astype(BF16).astype(F32)
    return hi, x - hi


def split3(x):
    hi = x.astype(BF16).astype(F32)
    rest = x - hi
    mid = rest.astype(BF16).astype(F32)
    return hi, mid, rest - mid


def kernel(
    gx_size, gy_size, rows, dims,
    field_hbm, points_hbm, weight_hbm, group_hbm,
    moments_ref,
    fv, send_rows, recv_rows, send_cols, recv_cols, send_corners, recv_corners,
    lnat, left, cols_t, halo_l, rhs_f, rhs, node_w, csc,
    cells0, cells1, kept, aside, part, both, acc, nat, mine, theirs,
    points_ref, weight_ref, group_ref,
    load_sem, send_sem, recv_sem,
):
    ext = rows + 2 * HALO
    quads = ext // ROWS
    modes = dims + 1
    fields = 4 * modes
    ring = LANES + 2 * HALO
    chunk = ring // SUBLANES
    kpad = 40
    groups = kpad // SUBLANES
    core = lax.axis_index("nodes")
    gx = lax.axis_index("gx")
    gy = lax.axis_index("gy")
    xn, xp = lax.rem(gx + 1, gx_size), lax.rem(gx + gx_size - 1, gx_size)
    yn, yp = lax.rem(gy + 1, gy_size), lax.rem(gy + gy_size - 1, gy_size)
    around = [
        (core, xp, gy), (core, xn, gy), (core, gx, yp), (core, gx, yn),
        (1 - core, gx, gy),
    ]

    barrier = pltpu.get_barrier_semaphore()
    for device in around:
        pl.semaphore_signal(barrier, inc=1, device_id=device, device_id_type=MESH)

    apart = fv.shape[0] // kpad

    @pl.loop(0, fields)
    def _(k):
        pltpu.make_async_copy(
            field_hbm.at[pl.ds(k * rows, rows)], fv.at[pl.ds(k * apart, rows)], load_sem.at[0]
        ).start()

    small = [
        pltpu.make_async_copy(source, target, load_sem.at[1 + i])
        for i, (source, target) in enumerate(
            [(points_hbm, points_ref), (weight_hbm, weight_ref), (group_hbm, group_ref)]
        )
    ]
    for copy in small:
        copy.start()
    fv[pl.ds(fields * apart, (kpad - fields) * apart), :] = jnp.zeros(((kpad - fields) * apart, LANES), F32)

    for copy in small:
        copy.wait()
    count = group_ref.shape[0]
    included = (group_ref[...].reshape(1, count) < 2).astype(F32)
    weights = weight_ref[...].reshape(1, count)
    weight_total = jnp.sum(weights * included, axis=1, keepdims=True)
    row8 = lax.broadcasted_iota(jnp.int32, (SUBLANES, LANES), 0)
    blocks = count // LANES
    pieces = [included[:, b * LANES : (b + 1) * LANES] for b in range(blocks)]
    stacked = jnp.zeros((SUBLANES, LANES), F32)
    for b in range(blocks):
        stacked = jnp.where(row8 == b, jnp.broadcast_to(pieces[b], (SUBLANES, LANES)), stacked)
    before = lax.broadcasted_iota(jnp.int32, (LANES, LANES), 0) <= lax.broadcasted_iota(jnp.int32, (LANES, LANES), 1)
    within = nn(stacked.astype(BF16), before.astype(F32).astype(BF16))
    totals = jnp.sum(stacked, axis=1, keepdims=True)
    slot = (lax.broadcasted_iota(jnp.int32, (SLOTS, LANES), 0) + (core * SLOTS + 1)).astype(F32)
    offset = jnp.zeros((1, 1), F32)
    chosen = []
    for b in range(blocks):
        order = within[b : b + 1] + offset
        offset = offset + totals[b : b + 1]
        order = jnp.where(pieces[b] > 0, order, 0.0)
        chosen.append(jnp.where(slot == jnp.broadcast_to(order, (SLOTS, LANES)), 1.0, 0.0).astype(BF16))
    select = jnp.concatenate(chosen, axis=1)
    w_hi, w_mid, w_lo = split3(weights)
    w_rows = lax.broadcasted_iota(jnp.int32, (SUBLANES, count), 0)
    w_stack = jnp.where(w_rows == 0, w_hi, jnp.where(w_rows == 1, w_mid, jnp.where(w_rows == 2, w_lo, 0.0)))
    found = nt(jnp.concatenate([*split3(points_ref[...]), w_stack], axis=0).astype(BF16), select)
    coords = found[0:dims] + found[dims : 2 * dims] + found[2 * dims : 3 * dims]
    held = found[3 * dims : 3 * dims + 1] + found[3 * dims + 1 : 3 * dims + 2] + found[3 * dims + 2 : 3 * dims + 3]
    node_w[...] = jnp.broadcast_to(held, (SUBLANES, SLOTS))

    csc[0:1, :] = jnp.ones((1, SLOTS), F32)
    csc[1 : 1 + dims, :] = coords
    coefficient = csc[...][0:modes]
    rhs_f[...] = jnp.zeros_like(rhs_f)

    def place(group, half, h, field, scale):
        hi, lo = split2(coefficient[:, h * LANES : (h + 1) * LANES] * scale)
        at = field * modes
        lanes = pl.ds(half * LANES, LANES)
        rhs_f[group, pl.ds(at, modes), lanes] = hi
        rhs_f[group, pl.ds(kpad + at, modes), lanes] = lo
        rhs_f[group, pl.ds(2 * kpad + at, modes), lanes] = hi

    for h in range(2):
        for k in range(4):
            place(2 * h + k // 2, k % 2, h, 3, TIME_STEP)
            place(2 * h + k // 2, k % 2, h, 1 + k // 2, (0.5, -0.5, -0.5, 0.5)[k] * TIME_STEP)
        place(4, h, h, 0, 1.0)
    rhs[...] = rhs_f[...].astype(BF16)

    rest = jnp.zeros((SUBLANES, LANES), F32)

    def turned(x):
        hi, lo = split2(x)
        stack = jnp.concatenate([hi, hi, lo, rest], axis=0).astype(BF16)
        return jnp.transpose(stack).astype(F32)

    top = rows + HALO - 1

    def turn_rows(quad):
        for k in range(ROWS):
            x = fv[pl.ds(top - ROWS * quad - k, kpad, stride=apart), :]
            lnat[lax.rem(quad, 2), pl.ds(k * ring, LANES), :] = turned(x)

    planes = (cells0, cells1)

    def targets(group):
        if group == 4:
            return [lambda row: planes[0].at[row, 4], lambda row: planes[1].at[row, 4]]
        return [
            lambda row: planes[group // 2].at[row, 2 * (group % 2)],
            lambda row: planes[group // 2].at[row, 2 * (group % 2) + 1],
        ]

    def parameters(quad):
        slot = lax.rem(quad, 2)
        cells = []
        for k in range(ROWS):
            cells += [lnat[slot, pl.ds(k * ring + j, SUBLANES, stride=chunk), :] for j in range(chunk)]
        left[...] = jnp.concatenate(cells, axis=0).astype(BF16)
        for group in range(5):
            found = nn(left[...], rhs[group])
            for half, target in enumerate(targets(group)):
                for k in range(ROWS):
                    piece = found[k * ring : (k + 1) * ring, half * LANES : (half + 1) * LANES]
                    target(ROWS * quad + k)[...] = piece

    sent = fields * HALO
    for side in range(2):
        recv_rows[side, pl.ds(sent, kpad * HALO - sent), :] = jnp.zeros((kpad * HALO - sent, LANES), F32)
    acc[...] = jnp.zeros_like(acc)
    pltpu.make_async_copy(field_hbm, fv.at[pl.ds(0, fields * rows)], load_sem.at[0]).wait()

    lane = lax.broadcasted_iota(jnp.int32, (SUBLANES, LANES), 1)
    by_halo = lane // HALO
    block = HALO * HALO
    by_block = lane // block
    per_tile = LANES // HALO
    tiles = rows // per_tile

    for r in range(HALO):
        send_rows[0, pl.ds(r, kpad, stride=HALO), :] = fv[pl.ds(r, kpad, stride=apart), :]
        send_rows[1, pl.ds(r, kpad, stride=HALO), :] = fv[pl.ds(rows - HALO + r, kpad, stride=apart), :]
    for t in range(tiles):
        low = [jnp.zeros((SUBLANES, LANES), F32)] * groups
        high = [jnp.zeros((SUBLANES, LANES), F32)] * groups
        for g in range(per_tile):
            at_high = by_halo == g
            at_low = by_halo == (g + 1) % per_tile
            for m in range(groups):
                x = fv[pl.ds(m * SUBLANES * apart + t * per_tile + g, SUBLANES, stride=apart), :]
                x = pltpu.roll(x, (HALO * (g + 1)) % LANES, 1)
                high[m] = jnp.where(at_high, x, high[m])
                low[m] = jnp.where(at_low, x, low[m])
        for side, values in enumerate((low, high)):
            for m in range(groups):
                send_cols[side, t, m * SUBLANES : (m + 1) * SUBLANES, :] = values[m]

    turn_rows(1)

    @pl.loop(1, 1 + EARLY)
    def _(quad):
        parameters(quad)
        turn_rows(quad + 1)

    pl.semaphore_wait(barrier, len(around))

    def remote(index, source, target, device):
        copy = pltpu.make_async_remote_copy(
            src_ref=source, dst_ref=target,
            send_sem=send_sem.at[index], recv_sem=recv_sem.at[index],
            device_id=device, device_id_type=MESH,
        )
        copy.start()
        return copy

    copies = [
        remote(2, send_cols.at[0], recv_cols.at[0], (core, gx, yp)),
        remote(3, send_cols.at[1], recv_cols.at[1], (core, gx, yn)),
        remote(0, send_rows.at[0, pl.ds(0, sent)], recv_rows.at[0, pl.ds(0, sent)], (core, xp, gy)),
        remote(1, send_rows.at[1, pl.ds(0, sent)], recv_rows.at[1, pl.ds(0, sent)], (core, xn, gy)),
    ]

    @pl.loop(1 + EARLY, quads - 2)
    def _(quad):
        parameters(quad)
        turn_rows(quad + 1)

    parameters(quads - 2)

    edge = (chunk - SUBLANES) * SUBLANES + SUBLANES - 1

    def halo_rows(side, quad):
        for k in range(ROWS):
            row = top - (ROWS * quad + k)
            x = recv_rows[side, pl.ds(row - rows if side == 0 else row + HALO, kpad, stride=HALO), :]
            lnat[quad % 2, pl.ds(k * ring, LANES), :] = turned(x)
        parameters(quad)

    def fill(e, right, left_side):
        halo_l[pl.ds(e * SUBLANES, HALO), :] = cols_t[pl.ds(right, HALO), :]
        halo_l[pl.ds(e * SUBLANES + HALO, HALO), :] = cols_t[pl.ds(left_side, HALO), :]

    def patch(first, number):
        cells = halo_l[pl.ds(first * SUBLANES, number * SUBLANES), :].astype(BF16)
        for group in range(5):
            found = nn(cells, rhs[group])
            for half, target in enumerate(targets(group)):
                for k in range(number):
                    piece = found[k * SUBLANES : (k + 1) * SUBLANES, half * LANES : (half + 1) * LANES]
                    target(first + k)[pl.ds(edge, SUBLANES, stride=SUBLANES), :] = piece

    for copy in copies[:2]:
        copy.wait_recv()
    for t in range(2 * tiles):
        cols_t[pl.ds(t * LANES, LANES), :] = turned(recv_cols[t // tiles, t % tiles])
    for row in range(rows):
        t, g = divmod(row, per_tile)
        fill(top - row, t * LANES + HALO * ((g + 1) % per_tile), (tiles + t) * LANES + HALO * g)
    patch(HALO, rows)

    for copy in copies[2:]:
        copy.wait_recv()
    for side in range(2):
        low = jnp.zeros((SUBLANES, LANES), F32)
        high = jnp.zeros((SUBLANES, LANES), F32)
        for m in range(groups):
            for r in range(HALO):
                x = recv_rows[side, pl.ds(m * SUBLANES * HALO + r, SUBLANES, stride=HALO), :]
                at = block * m + HALO * r
                mask = by_halo == at // HALO
                low = jnp.where(mask, pltpu.roll(x, at, 1) if at else x, low)
                high = jnp.where(mask, pltpu.roll(x, at + HALO, 1), high)
        send_corners[2 * side] = low
        send_corners[2 * side + 1] = high
    corner_copies = [
        remote(4, send_corners.at[0], recv_corners.at[0], (core, gx, yp)),
        remote(5, send_corners.at[1], recv_corners.at[1], (core, gx, yn)),
        remote(6, send_corners.at[2], recv_corners.at[2], (core, gx, yp)),
        remote(7, send_corners.at[3], recv_corners.at[3], (core, gx, yn)),
    ]

    def halo_ends():
        halo_rows(0, 0)
        halo_rows(1, quads - 1)
        for copy in corner_copies:
            copy.wait_recv()
        corners = [recv_corners[k] for k in range(4)]
        unpacked = []
        for m in range(groups):
            x = jnp.zeros((SUBLANES, LANES), F32)
            for k in range(4):
                x = jnp.where(by_block == k, pltpu.roll(corners[k], block * (k - m) % LANES, 1), x)
            unpacked.append(x)
        corner = 2 * tiles * LANES
        cols_t[pl.ds(corner, LANES), :] = turned(jnp.concatenate(unpacked, axis=0))
        for r in range(HALO):
            fill(top - rows - r, corner + HALO * r, corner + block + HALO * r)
            fill(top + HALO - r, corner + 2 * block + HALO * r, corner + 3 * block + HALO * r)
        patch(0, HALO)
        patch(ext - HALO, HALO)

    tile = [pl.ds(SUBLANES * j, SUBLANES) for j in range(chunk)]

    def advance(step, h, plane, skip, beyond=None):
        cells = [kept.at[h]] + [plane.at[skip + k, 4] for k in range(ROWS)]
        cells.append(plane.at[skip + ROWS, 4] if beyond is None else beyond)

        def column(j):
            return [ref[tile[j], :] for ref in cells]

        column_now = column(0)
        last = [ref[tile[chunk - 1], :] for ref in cells[1:-1]]
        wrap = [column_now[k + 1] - pltpu.roll(last[k], 1, 0) for k in range(ROWS)]
        south = wrap
        for j in range(chunk):
            if j + 1 < chunk:
                column_next = column(j + 1)
                north = [column_next[k + 1] - column_now[k + 1] for k in range(ROWS)]
            else:
                column_next = None
                north = [pltpu.roll(x, SUBLANES - 1, 0) for x in wrap]
            east = [column_now[k + 1] - column_now[k] for k in range(ROWS + 1)]
            for k in range(ROWS):
                c = [plane[skip + k, m, tile[j], :] for m in range(4)]
                new = column_now[k + 1] + (
                    (c[0] * east[k + 1] - c[1] * east[k]) + (c[2] * north[k] - c[3] * south[k])
                )
                if step < 4:
                    plane[skip + k, 4, tile[j], :] = new
                    continue
                one = node_w[:, h * LANES : (h + 1) * LANES] * new
                two = one * new
                if h == 0:
                    part[k, 0, tile[j], :] = one
                    part[k, 1, tile[j], :] = two
                else:
                    both[k, 0, tile[j], :] = one + part[k, 0, tile[j], :]
                    both[k, 1, tile[j], :] = two + part[k, 1, tile[j], :]
            kept[h, tile[j], :] = column_now[ROWS]
            column_now, south = column_next, north

    def gather_sums(first):
        masks = [(lane == top - first - k + m * rows, k, m) for k in range(ROWS) for m in range(2)]
        for j in range(chunk):
            old = acc[tile[j], :]
            for mask, k, m in masks:
                old = jnp.where(mask, jnp.sum(both[k, m, tile[j], :], axis=1, keepdims=True), old)
            acc[tile[j], :] = old

    inner = HALO + 1
    spans = {1: (inner, (rows - 2) // ROWS), 2: (2, quads - 1), 3: (1, quads - 1), 4: (HALO, quads - 2)}
    for step, (start, turns) in spans.items():
        for h in range(2):
            kept[h] = planes[h][start - 1, 4]
            if step == 1:
                aside[h] = planes[h][start, 4]
        if step == 4:
            both[...] = jnp.zeros_like(both)

        def run(first):
            if step == 4:
                gather_sums(first - ROWS)
            for h in range(2):
                advance(step, h, planes[h].at[pl.ds(first, ROWS + 1)], 0)

        @pl.loop(0, turns)
        def _(turn):
            run(start + ROWS * turn)

        if step == 1:
            halo_ends()
            for first in range(start + ROWS * turns, ext - 1, ROWS):
                run(first)
            for h in range(2):
                kept[h] = planes[h][0, 4]
                advance(step, h, planes[h].at[pl.ds(1, ROWS + 1)], 0, aside.at[h])

    gather_sums(rows + HALO - ROWS)

    for j in range(chunk):
        nat[pl.ds(j, SUBLANES, stride=chunk), :] = acc[tile[j], :]
    mine[...] = jnp.transpose(nat[0:LANES, :])
    swap = remote(8, mine, theirs, (1 - core, gx, gy))
    for copy in copies + corner_copies:
        copy.wait_send()
    swap.wait()
    moments_ref[...] = (mine[...] + theirs[...]) / weight_total


def on_device(mesh, field_modes, node_points, quad_weight, group_of):
    rows, cols = field_modes.shape[2:]
    count, dims = node_points.shape
    modes = dims + 1
    ext = rows + 2 * HALO
    ring = cols + 2 * HALO
    kpad = 40
    tiles = rows * HALO // LANES
    vmem = pl.BlockSpec(memory_space=pltpu.VMEM)
    moments = pl.pallas_call(
        functools.partial(kernel, mesh.shape["gx"], mesh.shape["gy"], rows, dims),
        out_shape=pltpu.VMEM((2 * rows, cols), F32),
        in_specs=[pl.BlockSpec(memory_space=pl.ANY)] * 4,
        out_specs=vmem,
        scratch_shapes=[
            pltpu.VMEM((kpad * (rows + SUBLANES), LANES), F32),
            pltpu.VMEM((2, kpad * HALO, LANES), F32),
            pltpu.VMEM((2, kpad * HALO, LANES), F32),
            pltpu.VMEM((2, tiles, kpad, LANES), F32),
            pltpu.VMEM((2, tiles, kpad, LANES), F32),
            pltpu.VMEM((4, SUBLANES, LANES), F32),
            pltpu.VMEM((4, SUBLANES, LANES), F32),
            pltpu.VMEM((2, ROWS * ring, LANES), F32),
            pltpu.VMEM((ROWS * ring, LANES), BF16),
            pltpu.VMEM(((2 * tiles + 1) * LANES, LANES), F32),
            pltpu.VMEM((ext * SUBLANES, LANES), F32),
            pltpu.VMEM((5, LANES, 2 * LANES), F32),
            pltpu.VMEM((5, LANES, 2 * LANES), BF16),
            pltpu.VMEM((SUBLANES, SLOTS), F32),
            pltpu.VMEM((2 * SUBLANES, SLOTS), F32),
            pltpu.VMEM((ext + 2, 5, ring, LANES), F32),
            pltpu.VMEM((ext + 2, 5, ring, LANES), F32),
            pltpu.VMEM((2, ring, LANES), F32),
            pltpu.VMEM((2, ring, LANES), F32),
            pltpu.VMEM((ROWS, 2, ring, LANES), F32),
            pltpu.VMEM((ROWS, 2, ring, LANES), F32),
            pltpu.VMEM((ring, LANES), F32),
            pltpu.VMEM((ring, LANES), F32),
            pltpu.VMEM((2 * rows, LANES), F32),
            pltpu.VMEM((2 * rows, LANES), F32),
            pltpu.VMEM((dims, count), F32),
            pltpu.VMEM((count,), F32),
            pltpu.VMEM((count,), jnp.int32),
            pltpu.SemaphoreType.DMA((4,)),
            pltpu.SemaphoreType.DMA((9,)),
            pltpu.SemaphoreType.DMA((9,)),
        ],
        compiler_params=pltpu.CompilerParams(
            collective_id=0, has_side_effects=True, vmem_limit_bytes=62 * 1024 * 1024
        ),
    )(
        field_modes.reshape(4 * modes * rows, cols),
        node_points.T,
        quad_weight,
        group_of,
    )
    mean_field = moments[:rows]
    return mean_field, moments[rows:] - mean_field * mean_field


def solution(mesh):
    return jax.shard_map(
        functools.partial(on_device, mesh),
        mesh=mesh,
        in_specs=(P(None, None, "gx", "gy"), P(), P(), P()),
        out_specs=(P("gx", "gy"), P("gx", "gy")),
        check_vma=False,
    )
```

```python
import functools

import jax
import jax.numpy as jnp
from jax import lax
from jax.experimental import pallas as pl
from jax.experimental.pallas import tpu as pltpu
from jax.sharding import PartitionSpec as P

TIME_STEP = 0.15
HALO = 4
LANES = 128
SUBLANES = 8
SLOTS = 256
ROWS = 4
EARLY = 4
MESH = pl.DeviceIdType.MESH
F32 = jnp.float32
BF16 = jnp.bfloat16


def nn(a, b):
    return lax.dot_general(a, b, (((1,), (0,)), ((), ())), preferred_element_type=F32)


def nt(a, b):
    return lax.dot_general(a, b, (((1,), (1,)), ((), ())), preferred_element_type=F32)


def split2(x):
    hi = x.astype(BF16).astype(F32)
    return hi, x - hi


def split3(x):
    hi = x.astype(BF16).astype(F32)
    rest = x - hi
    mid = rest.astype(BF16).astype(F32)
    return hi, mid, rest - mid


def kernel(
    gx_size, gy_size, rows, dims,
    field_hbm, points_hbm, weight_hbm, group_hbm,
    moments_ref,
    fv, send_rows, recv_rows, send_cols, recv_cols, send_corners, recv_corners,
    lnat, left, cols_t, halo_l, rhs_f, rhs, node_w, csc,
    cf0, cf1, ua, ub, kept, part, both, acc, nat, mine, theirs,
    points_ref, weight_ref, group_ref,
    load_sem, send_sem, recv_sem,
):
    ext = rows + 2 * HALO
    quads = ext // ROWS
    modes = dims + 1
    fields = 4 * modes
    ring = LANES + 2 * HALO
    chunk = ring // SUBLANES
    kpad = 40
    groups = kpad // SUBLANES
    core = lax.axis_index("nodes")
    gx = lax.axis_index("gx")
    gy = lax.axis_index("gy")
    xn, xp = lax.rem(gx + 1, gx_size), lax.rem(gx + gx_size - 1, gx_size)
    yn, yp = lax.rem(gy + 1, gy_size), lax.rem(gy + gy_size - 1, gy_size)
    around = [
        (core, xp, gy), (core, xn, gy), (core, gx, yp), (core, gx, yn),
        (core, xp, yp), (core, xp, yn), (core, xn, yp), (core, xn, yn),
        (1 - core, gx, gy),
    ]

    barrier = pltpu.get_barrier_semaphore()
    for device in around:
        pl.semaphore_signal(barrier, inc=1, device_id=device, device_id_type=MESH)

    apart = fv.shape[0] // kpad

    @pl.loop(0, fields)
    def _(k):
        pltpu.make_async_copy(
            field_hbm.at[pl.ds(k * rows, rows)], fv.at[pl.ds(k * apart, rows)], load_sem.at[0]
        ).start()

    small = [
        pltpu.make_async_copy(source, target, load_sem.at[1 + i])
        for i, (source, target) in enumerate(
            [(points_hbm, points_ref), (weight_hbm, weight_ref), (group_hbm, group_ref)]
        )
    ]
    for copy in small:
        copy.start()
    fv[pl.ds(fields * apart, (kpad - fields) * apart), :] = jnp.zeros(((kpad - fields) * apart, LANES), F32)

    for copy in small:
        copy.wait()
    count = group_ref.shape[0]
    included = (group_ref[...].reshape(1, count) < 2).astype(F32)
    weights = weight_ref[...].reshape(1, count)
    weight_total = jnp.sum(weights * included, axis=1, keepdims=True)
    row8 = lax.broadcasted_iota(jnp.int32, (SUBLANES, LANES), 0)
    blocks = count // LANES
    pieces = [included[:, b * LANES : (b + 1) * LANES] for b in range(blocks)]
    stacked = jnp.zeros((SUBLANES, LANES), F32)
    for b in range(blocks):
        stacked = jnp.where(row8 == b, jnp.broadcast_to(pieces[b], (SUBLANES, LANES)), stacked)
    before = lax.broadcasted_iota(jnp.int32, (LANES, LANES), 0) <= lax.broadcasted_iota(jnp.int32, (LANES, LANES), 1)
    within = nn(stacked.astype(BF16), before.astype(F32).astype(BF16))
    totals = jnp.sum(stacked, axis=1, keepdims=True)
    slot = (lax.broadcasted_iota(jnp.int32, (SLOTS, LANES), 0) + (core * SLOTS + 1)).astype(F32)
    offset = jnp.zeros((1, 1), F32)
    chosen = []
    for b in range(blocks):
        order = within[b : b + 1] + offset
        offset = offset + totals[b : b + 1]
        order = jnp.where(pieces[b] > 0, order, 0.0)
        chosen.append(jnp.where(slot == jnp.broadcast_to(order, (SLOTS, LANES)), 1.0, 0.0).astype(BF16))
    select = jnp.concatenate(chosen, axis=1)
    w_hi, w_mid, w_lo = split3(weights)
    w_rows = lax.broadcasted_iota(jnp.int32, (SUBLANES, count), 0)
    w_stack = jnp.where(w_rows == 0, w_hi, jnp.where(w_rows == 1, w_mid, jnp.where(w_rows == 2, w_lo, 0.0)))
    found = nt(jnp.concatenate([*split3(points_ref[...]), w_stack], axis=0).astype(BF16), select)
    coords = found[0:dims] + found[dims : 2 * dims] + found[2 * dims : 3 * dims]
    held = found[3 * dims : 3 * dims + 1] + found[3 * dims + 1 : 3 * dims + 2] + found[3 * dims + 2 : 3 * dims + 3]
    node_w[...] = jnp.broadcast_to(held, (SUBLANES, SLOTS))

    csc[0:1, :] = jnp.ones((1, SLOTS), F32)
    csc[1 : 1 + dims, :] = coords
    coefficient = csc[...][0:modes]
    rhs_f[...] = jnp.zeros_like(rhs_f)

    def place(group, half, h, field, scale):
        hi, lo = split2(coefficient[:, h * LANES : (h + 1) * LANES] * scale)
        at = field * modes
        lanes = pl.ds(half * LANES, LANES)
        rhs_f[group, pl.ds(at, modes), lanes] = hi
        rhs_f[group, pl.ds(kpad + at, modes), lanes] = lo
        rhs_f[group, pl.ds(2 * kpad + at, modes), lanes] = hi

    for h in range(2):
        for k in range(4):
            place(2 * h + k // 2, k % 2, h, 3, TIME_STEP)
            place(2 * h + k // 2, k % 2, h, 1 + k // 2, (-0.5, 0.5)[k % 2] * TIME_STEP)
        place(4, h, h, 0, 1.0)
    rhs[...] = rhs_f[...].astype(BF16)

    rest = jnp.zeros((SUBLANES, LANES), F32)

    def turned(x):
        hi, lo = split2(x)
        stack = jnp.concatenate([hi, hi, lo, rest], axis=0).astype(BF16)
        return jnp.transpose(stack).astype(F32)

    def turn_rows(quad):
        for k in range(ROWS):
            x = fv[pl.ds(ROWS * quad - HALO + k, kpad, stride=apart), :]
            lnat[lax.rem(quad, 2), pl.ds(k * ring, LANES), :] = turned(x)

    cfs, us = (cf0, cf1), (ua, ub)

    def targets(group):
        if group == 4:
            return [lambda row: us[0].at[row], lambda row: us[1].at[row]]
        return [
            lambda row: cfs[group // 2].at[row, 2 * (group % 2)],
            lambda row: cfs[group // 2].at[row, 2 * (group % 2) + 1],
        ]

    def parameters(quad):
        slot = lax.rem(quad, 2)
        cells = []
        for k in range(ROWS):
            cells += [lnat[slot, pl.ds(k * ring + j, SUBLANES, stride=chunk), :] for j in range(chunk)]
        left[...] = jnp.concatenate(cells, axis=0).astype(BF16)
        for group in range(5):
            found = nn(left[...], rhs[group])
            for half, target in enumerate(targets(group)):
                for k in range(ROWS):
                    piece = found[k * ring : (k + 1) * ring, half * LANES : (half + 1) * LANES]
                    target(ROWS * quad + k)[...] = piece

    near = HALO - 1
    sent = kpad * near
    for side in range(2):
        recv_rows[side, pl.ds(sent, SUBLANES), :] = jnp.zeros((SUBLANES, LANES), F32)
    acc[...] = jnp.zeros_like(acc)
    pltpu.make_async_copy(field_hbm, fv.at[pl.ds(0, fields * rows)], load_sem.at[0]).wait()

    lane = lax.broadcasted_iota(jnp.int32, (SUBLANES, LANES), 1)
    by_halo = lane // HALO
    block = HALO * HALO
    by_block = lane // block
    per_tile = LANES // HALO
    tiles = rows // per_tile

    for side in range(2):
        for r in range(near):
            row = r if side == 0 else rows - near + r
            send_rows[side, pl.ds(r, kpad, stride=near), :] = fv[pl.ds(row, kpad, stride=apart), :]
        row = near if side == 0 else rows - HALO
        send_rows[side, pl.ds(fields * near, modes), :] = fv[pl.ds(row, modes, stride=apart), :]
    for t in range(tiles):
        low = [jnp.zeros((SUBLANES, LANES), F32)] * groups
        high = [jnp.zeros((SUBLANES, LANES), F32)] * groups
        for g in range(per_tile):
            at_high = by_halo == g
            at_low = by_halo == (g + 1) % per_tile
            for m in range(groups):
                x = fv[pl.ds(m * SUBLANES * apart + t * per_tile + g, SUBLANES, stride=apart), :]
                x = pltpu.roll(x, (HALO * (g + 1)) % LANES, 1)
                high[m] = jnp.where(at_high, x, high[m])
                low[m] = jnp.where(at_low, x, low[m])
        for side, values in enumerate((low, high)):
            for m in range(groups):
                send_cols[side, t, m * SUBLANES : (m + 1) * SUBLANES, :] = values[m]
            for end in range(2):
                if t != (0, tiles - 1)[end]:
                    continue
                at = HALO * (1 - side) + (0, LANES - block)[end]
                packed = jnp.zeros((SUBLANES, LANES), F32)
                for m in range(groups):
                    packed = jnp.where(by_block == m, pltpu.roll(values[m], (block * m - at) % LANES, 1), packed)
                send_corners[2 * end + side] = packed

    turn_rows(1)

    @pl.loop(1, 1 + EARLY)
    def _(quad):
        parameters(quad)
        turn_rows(quad + 1)

    pl.semaphore_wait(barrier, len(around))

    def remote(index, source, target, device):
        copy = pltpu.make_async_remote_copy(
            src_ref=source, dst_ref=target,
            send_sem=send_sem.at[index], recv_sem=recv_sem.at[index],
            device_id=device, device_id_type=MESH,
        )
        copy.start()
        return copy

    copies = [
        remote(4, send_corners.at[0], recv_corners.at[0], (core, xp, yp)),
        remote(5, send_corners.at[1], recv_corners.at[1], (core, xp, yn)),
        remote(6, send_corners.at[2], recv_corners.at[2], (core, xn, yp)),
        remote(7, send_corners.at[3], recv_corners.at[3], (core, xn, yn)),
        remote(0, send_rows.at[0, pl.ds(0, sent)], recv_rows.at[0, pl.ds(0, sent)], (core, xp, gy)),
        remote(1, send_rows.at[1, pl.ds(0, sent)], recv_rows.at[1, pl.ds(0, sent)], (core, xn, gy)),
        remote(2, send_cols.at[0], recv_cols.at[0], (core, gx, yp)),
        remote(3, send_cols.at[1], recv_cols.at[1], (core, gx, yn)),
    ]

    @pl.loop(1 + EARLY, quads - 2)
    def _(quad):
        parameters(quad)
        turn_rows(quad + 1)

    parameters(quads - 2)

    for copy in copies:
        copy.wait_recv()

    for side, quad in ((1, 0), (0, quads - 1)):
        for k in range(ROWS):
            outer = k == (near if side == 0 else 0)
            if outer:
                x = recv_rows[side, pl.ds(fields * near, 2 * SUBLANES), :]
                x = jnp.concatenate([x, jnp.zeros((kpad - 2 * SUBLANES, LANES), F32)], axis=0)
            else:
                x = recv_rows[side, pl.ds(k - side, kpad, stride=near), :]
            lnat[quad % 2, pl.ds(k * ring, LANES), :] = turned(x)
        parameters(quad)

    for t in range(2 * tiles):
        cols_t[pl.ds(t * LANES, LANES), :] = turned(recv_cols[t // tiles, t % tiles])
    corners = [recv_corners[k] for k in range(4)]
    unpacked = []
    for m in range(groups):
        x = jnp.zeros((SUBLANES, LANES), F32)
        for k in range(4):
            x = jnp.where(by_block == k, pltpu.roll(corners[k], block * (k - m) % LANES, 1), x)
        unpacked.append(x)
    cols_t[pl.ds(2 * tiles * LANES, LANES), :] = turned(jnp.concatenate(unpacked, axis=0))

    def column_halo(row, right, left_side):
        halo_l[pl.ds(row * SUBLANES, HALO), :] = cols_t[pl.ds(right, HALO), :]
        halo_l[pl.ds(row * SUBLANES + HALO, HALO), :] = cols_t[pl.ds(left_side, HALO), :]

    for row in range(rows):
        t, g = divmod(row, per_tile)
        column_halo(
            row + HALO,
            t * LANES + HALO * ((g + 1) % per_tile),
            (tiles + t) * LANES + HALO * g,
        )
    corner = 2 * tiles * LANES
    for r in range(HALO):
        column_halo(rows + HALO + r, corner + HALO * r, corner + block + HALO * r)
        column_halo(r, corner + 2 * block + HALO * r, corner + 3 * block + HALO * r)
    edge = (chunk - SUBLANES) * SUBLANES + SUBLANES - 1
    for group in range(5):
        found = nn(halo_l[...].astype(BF16), rhs[group])
        for half, target in enumerate(targets(group)):
            for row in range(ext):
                piece = found[row * SUBLANES : (row + 1) * SUBLANES, half * LANES : (half + 1) * LANES]
                target(row)[pl.ds(edge, SUBLANES, stride=SUBLANES), :] = piece

    tile = [pl.ds(SUBLANES * j, SUBLANES) for j in range(chunk)]

    def advance(step, h, first, number):
        cf = cfs[h].at[pl.ds(first, number)]
        u = us[h].at[pl.ds(first, number + 1)]
        cells = [kept.at[h]] + [u.at[k] for k in range(number + 1)]

        def column(j):
            return [ref[tile[j], :] for ref in cells]

        column_now = column(0)
        last = [ref[tile[chunk - 1], :] for ref in cells[1:-1]]
        wrap = [column_now[k + 1] - pltpu.roll(last[k], 1, 0) for k in range(number)]
        south = wrap
        for j in range(chunk):
            if j + 1 < chunk:
                column_next = column(j + 1)
                north = [column_next[k + 1] - column_now[k + 1] for k in range(number)]
            else:
                column_next = None
                north = [pltpu.roll(x, SUBLANES - 1, 0) for x in wrap]
            east = [column_now[k + 1] - column_now[k] for k in range(number + 1)]
            for k in range(number):
                c = [cf[k, m, tile[j], :] for m in range(4)]
                new = column_now[k + 1] + (
                    (c[0] * east[k + 1] - c[1] * east[k]) + (c[2] * north[k] - c[3] * south[k])
                )
                if step < 4:
                    u[k, tile[j], :] = new
                    continue
                one = node_w[:, h * LANES : (h + 1) * LANES] * new
                two = one * new
                if h == 0:
                    part[k, 0, tile[j], :] = one
                    part[k, 1, tile[j], :] = two
                else:
                    both[k, 0, tile[j], :] = one + part[k, 0, tile[j], :]
                    both[k, 1, tile[j], :] = two + part[k, 1, tile[j], :]
            kept[h, tile[j], :] = column_now[number]
            column_now, south = column_next, north

    def gather_sums(first):
        masks = [(lane == first + k + m * rows, k, m) for k in range(ROWS) for m in range(2)]
        for j in range(chunk):
            old = acc[tile[j], :]
            for mask, k, m in masks:
                old = jnp.where(mask, jnp.sum(both[k, m, tile[j], :], axis=1, keepdims=True), old)
            acc[tile[j], :] = old

    for step in range(1, 5):
        start, needed = step, ext - 2 * step
        for h in range(2):
            kept[h] = us[h][max(start - 1, 0)]
        if step == 4:
            both[...] = jnp.zeros_like(both)

        @pl.loop(0, needed // ROWS)
        def _(turn):
            first = start + ROWS * turn
            if step == 4:
                gather_sums(first - HALO - ROWS)
            for h in range(2):
                advance(step, h, first, ROWS)

        if needed % ROWS:
            for h in range(2):
                advance(step, h, start + needed // ROWS * ROWS, needed % ROWS)

    gather_sums(rows - ROWS)

    for j in range(chunk):
        nat[pl.ds(j, SUBLANES, stride=chunk), :] = acc[tile[j], :]
    mine[...] = jnp.transpose(nat[0:LANES, :])
    swap = remote(8, mine, theirs, (1 - core, gx, gy))
    for copy in copies:
        copy.wait_send()
    swap.wait()
    moments_ref[...] = (mine[...] + theirs[...]) / weight_total


def on_device(mesh, field_modes, node_points, quad_weight, group_of):
    rows, cols = field_modes.shape[2:]
    count, dims = node_points.shape
    modes = dims + 1
    ext = rows + 2 * HALO
    ring = cols + 2 * HALO
    kpad = 40
    tiles = rows * HALO // LANES
    vmem = pl.BlockSpec(memory_space=pltpu.VMEM)
    moments = pl.pallas_call(
        functools.partial(kernel, mesh.shape["gx"], mesh.shape["gy"], rows, dims),
        out_shape=pltpu.VMEM((2 * rows, cols), F32),
        in_specs=[pl.BlockSpec(memory_space=pl.ANY)] * 4,
        out_specs=vmem,
        scratch_shapes=[
            pltpu.VMEM((kpad * (rows + SUBLANES), LANES), F32),
            pltpu.VMEM((2, kpad * (HALO - 1) + SUBLANES, LANES), F32),
            pltpu.VMEM((2, kpad * (HALO - 1) + SUBLANES, LANES), F32),
            pltpu.VMEM((2, tiles, kpad, LANES), F32),
            pltpu.VMEM((2, tiles, kpad, LANES), F32),
            pltpu.VMEM((4, SUBLANES, LANES), F32),
            pltpu.VMEM((4, SUBLANES, LANES), F32),
            pltpu.VMEM((2, ROWS * ring, LANES), F32),
            pltpu.VMEM((ROWS * ring, LANES), BF16),
            pltpu.VMEM(((2 * tiles + 1) * LANES, LANES), F32),
            pltpu.VMEM((ext * SUBLANES, LANES), F32),
            pltpu.VMEM((5, LANES, 2 * LANES), F32),
            pltpu.VMEM((5, LANES, 2 * LANES), BF16),
            pltpu.VMEM((SUBLANES, SLOTS), F32),
            pltpu.VMEM((2 * SUBLANES, SLOTS), F32),
            pltpu.VMEM((ext, 4, ring, LANES), F32),
            pltpu.VMEM((ext, 4, ring, LANES), F32),
            pltpu.VMEM((ext + 1, ring, LANES), F32),
            pltpu.VMEM((ext + 1, ring, LANES), F32),
            pltpu.VMEM((2, ring, LANES), F32),
            pltpu.VMEM((ROWS, 2, ring, LANES), F32),
            pltpu.VMEM((ROWS, 2, ring, LANES), F32),
            pltpu.VMEM((ring, LANES), F32),
            pltpu.VMEM((ring, LANES), F32),
            pltpu.VMEM((2 * rows, LANES), F32),
            pltpu.VMEM((2 * rows, LANES), F32),
            pltpu.VMEM((dims, count), F32),
            pltpu.VMEM((count,), F32),
            pltpu.VMEM((count,), jnp.int32),
            pltpu.SemaphoreType.DMA((4,)),
            pltpu.SemaphoreType.DMA((9,)),
            pltpu.SemaphoreType.DMA((9,)),
        ],
        compiler_params=pltpu.CompilerParams(
            collective_id=0, has_side_effects=True, vmem_limit_bytes=62 * 1024 * 1024
        ),
    )(
        field_modes.reshape(4 * modes * rows, cols),
        node_points.T,
        quad_weight,
        group_of,
    )
    mean_field = moments[:rows]
    return mean_field, moments[rows:] - mean_field * mean_field


def solution(mesh):
    return jax.shard_map(
        functools.partial(on_device, mesh),
        mesh=mesh,
        in_specs=(P(None, None, "gx", "gy"), P(), P(), P()),
        out_specs=(P("gx", "gy"), P("gx", "gy")),
        check_vma=False,
    )
```

```python
import functools

import jax
import jax.numpy as jnp
from jax import lax
from jax.experimental import pallas as pl
from jax.experimental.pallas import tpu as pltpu
from jax.sharding import PartitionSpec as P

TIME_STEP = 0.15
HALO = 4
LANES = 128
SUBLANES = 8
SLOTS = 256
ROWS = 4
EARLY = 14
RING = 4
MESH = pl.DeviceIdType.MESH
F32 = jnp.float32
BF16 = jnp.bfloat16


def nn(a, b):
    return lax.dot_general(a, b, (((1,), (0,)), ((), ())), preferred_element_type=F32)


def nt(a, b):
    return lax.dot_general(a, b, (((1,), (1,)), ((), ())), preferred_element_type=F32)


def split2(x):
    hi = x.astype(BF16).astype(F32)
    return hi, x - hi


def split3(x):
    hi = x.astype(BF16).astype(F32)
    rest = x - hi
    mid = rest.astype(BF16).astype(F32)
    return hi, mid, rest - mid


def kernel(
    gx_size, gy_size, rows, dims,
    field_hbm, points_hbm, weight_hbm, group_hbm,
    moments_ref,
    fv, send_rows, recv_rows, send_cols, recv_cols, send_corners, recv_corners,
    lnat, left, cols_t, halo_l, rhs_f, rhs, node_w, csc,
    cf0, cf1, ua, ub, kept, part, both, acc, nat, mine, theirs,
    points_ref, weight_ref, group_ref,
    load_sem, send_sem, recv_sem,
):
    ext = rows + 2 * HALO
    quads = ext // ROWS
    modes = dims + 1
    fields = 4 * modes
    ring = LANES + 2 * HALO
    chunk = ring // SUBLANES
    kpad = 40
    groups = kpad // SUBLANES
    core = lax.axis_index("nodes")
    gx = lax.axis_index("gx")
    gy = lax.axis_index("gy")
    xn, xp = lax.rem(gx + 1, gx_size), lax.rem(gx + gx_size - 1, gx_size)
    yn, yp = lax.rem(gy + 1, gy_size), lax.rem(gy + gy_size - 1, gy_size)
    around = [
        (core, xp, gy), (core, xn, gy), (core, gx, yp), (core, gx, yn),
        (core, xp, yp), (core, xp, yn), (core, xn, yp), (core, xn, yn),
        (1 - core, gx, gy),
    ]

    barrier = pltpu.get_barrier_semaphore()
    for device in around:
        pl.semaphore_signal(barrier, inc=1, device_id=device, device_id_type=MESH)

    apart = fv.shape[0] // kpad

    @pl.loop(0, fields)
    def _(k):
        pltpu.make_async_copy(
            field_hbm.at[pl.ds(k * rows, rows)], fv.at[pl.ds(k * apart, rows)], load_sem.at[0]
        ).start()

    small = [
        pltpu.make_async_copy(source, target, load_sem.at[1 + i])
        for i, (source, target) in enumerate(
            [(points_hbm, points_ref), (weight_hbm, weight_ref), (group_hbm, group_ref)]
        )
    ]
    for copy in small:
        copy.start()
    fv[pl.ds(fields * apart, (kpad - fields) * apart), :] = jnp.zeros(((kpad - fields) * apart, LANES), F32)

    for copy in small:
        copy.wait()
    count = group_ref.shape[0]
    included = (group_ref[...].reshape(1, count) < 2).astype(F32)
    weights = weight_ref[...].reshape(1, count)
    weight_total = jnp.sum(weights * included, axis=1, keepdims=True)
    row8 = lax.broadcasted_iota(jnp.int32, (SUBLANES, LANES), 0)
    blocks = count // LANES
    pieces = [included[:, b * LANES : (b + 1) * LANES] for b in range(blocks)]
    stacked = jnp.zeros((SUBLANES, LANES), F32)
    for b in range(blocks):
        stacked = jnp.where(row8 == b, jnp.broadcast_to(pieces[b], (SUBLANES, LANES)), stacked)
    before = lax.broadcasted_iota(jnp.int32, (LANES, LANES), 0) <= lax.broadcasted_iota(jnp.int32, (LANES, LANES), 1)
    within = nn(stacked.astype(BF16), before.astype(F32).astype(BF16))
    totals = jnp.sum(stacked, axis=1, keepdims=True)
    slot = (lax.broadcasted_iota(jnp.int32, (SLOTS, LANES), 0) + (core * SLOTS + 1)).astype(F32)
    offset = jnp.zeros((1, 1), F32)
    chosen = []
    for b in range(blocks):
        order = within[b : b + 1] + offset
        offset = offset + totals[b : b + 1]
        order = jnp.where(pieces[b] > 0, order, 0.0)
        chosen.append(jnp.where(slot == jnp.broadcast_to(order, (SLOTS, LANES)), 1.0, 0.0).astype(BF16))
    select = jnp.concatenate(chosen, axis=1)
    w_hi, w_mid, w_lo = split3(weights)
    w_rows = lax.broadcasted_iota(jnp.int32, (SUBLANES, count), 0)
    w_stack = jnp.where(w_rows == 0, w_hi, jnp.where(w_rows == 1, w_mid, jnp.where(w_rows == 2, w_lo, 0.0)))
    found = nt(jnp.concatenate([*split3(points_ref[...]), w_stack], axis=0).astype(BF16), select)
    coords = found[0:dims] + found[dims : 2 * dims] + found[2 * dims : 3 * dims]
    held = found[3 * dims : 3 * dims + 1] + found[3 * dims + 1 : 3 * dims + 2] + found[3 * dims + 2 : 3 * dims + 3]
    node_w[...] = jnp.broadcast_to(held, (SUBLANES, SLOTS))

    csc[0:1, :] = jnp.ones((1, SLOTS), F32)
    csc[1 : 1 + dims, :] = coords
    coefficient = csc[...][0:modes]
    rhs_f[...] = jnp.zeros_like(rhs_f)

    def place(group, half, h, field, scale):
        hi, lo = split2(coefficient[:, h * LANES : (h + 1) * LANES] * scale)
        at = field * modes
        lanes = pl.ds(half * LANES, LANES)
        rhs_f[group, pl.ds(at, modes), lanes] = hi
        rhs_f[group, pl.ds(kpad + at, modes), lanes] = lo
        rhs_f[group, pl.ds(2 * kpad + at, modes), lanes] = hi

    for h in range(2):
        for k in range(4):
            place(2 * h + k // 2, k % 2, h, 3, TIME_STEP)
            place(2 * h + k // 2, k % 2, h, 1 + k // 2, (-0.5, 0.5)[k % 2] * TIME_STEP)
        place(4, h, h, 0, 1.0)
    rhs[...] = rhs_f[...].astype(BF16)

    rest = jnp.zeros((SUBLANES, LANES), F32)

    def turned(x):
        hi, lo = split2(x)
        stack = jnp.concatenate([hi, hi, lo, rest], axis=0).astype(BF16)
        return jnp.transpose(stack).astype(F32)

    def turn_rows(quad):
        for k in range(ROWS):
            x = fv[pl.ds(ROWS * quad - HALO + k, kpad, stride=apart), :]
            lnat[lax.rem(quad, 2), pl.ds(k * ring, LANES), :] = turned(x)

    cfs, us = (cf0, cf1), (ua, ub)

    def targets(group):
        if group == 4:
            return [lambda row: us[0].at[row], lambda row: us[1].at[row]]
        return [
            lambda row: cfs[group // 2].at[row, 2 * (group % 2)],
            lambda row: cfs[group // 2].at[row, 2 * (group % 2) + 1],
        ]

    def parameters(quad):
        slot = lax.rem(quad, 2)
        cells = []
        for k in range(ROWS):
            cells += [lnat[slot, pl.ds(k * ring + j, SUBLANES, stride=chunk), :] for j in range(chunk)]
        left[...] = jnp.concatenate(cells, axis=0).astype(BF16)
        for group in range(5):
            found = nn(left[...], rhs[group])
            for half, target in enumerate(targets(group)):
                for k in range(ROWS):
                    piece = found[k * ring : (k + 1) * ring, half * LANES : (half + 1) * LANES]
                    target(ROWS * quad + k)[...] = piece

    near = HALO - 1
    sent = kpad * near
    for side in range(2):
        recv_rows[side, pl.ds(sent, SUBLANES), :] = jnp.zeros((SUBLANES, LANES), F32)
    acc[...] = jnp.zeros_like(acc)
    pltpu.make_async_copy(field_hbm, fv.at[pl.ds(0, fields * rows)], load_sem.at[0]).wait()

    lane = lax.broadcasted_iota(jnp.int32, (SUBLANES, LANES), 1)
    by_halo = lane // HALO
    block = HALO * HALO
    by_block = lane // block
    per_tile = LANES // HALO
    tiles = rows // per_tile

    for side in range(2):
        for r in range(near):
            row = r if side == 0 else rows - near + r
            send_rows[side, pl.ds(r, kpad, stride=near), :] = fv[pl.ds(row, kpad, stride=apart), :]
        row = near if side == 0 else rows - HALO
        send_rows[side, pl.ds(fields * near, modes), :] = fv[pl.ds(row, modes, stride=apart), :]
    for t in range(tiles):
        low = [jnp.zeros((SUBLANES, LANES), F32)] * groups
        high = [jnp.zeros((SUBLANES, LANES), F32)] * groups
        for g in range(per_tile):
            at_high = by_halo == g
            at_low = by_halo == (g + 1) % per_tile
            for m in range(groups):
                x = fv[pl.ds(m * SUBLANES * apart + t * per_tile + g, SUBLANES, stride=apart), :]
                x = pltpu.roll(x, (HALO * (g + 1)) % LANES, 1)
                high[m] = jnp.where(at_high, x, high[m])
                low[m] = jnp.where(at_low, x, low[m])
        for side, values in enumerate((low, high)):
            for m in range(groups):
                send_cols[side, t, m * SUBLANES : (m + 1) * SUBLANES, :] = values[m]
            for end in range(2):
                if t != (0, tiles - 1)[end]:
                    continue
                at = HALO * (1 - side) + (0, LANES - block)[end]
                packed = jnp.zeros((SUBLANES, LANES), F32)
                for m in range(groups):
                    packed = jnp.where(by_block == m, pltpu.roll(values[m], (block * m - at) % LANES, 1), packed)
                send_corners[2 * end + side] = packed

    turn_rows(1)

    x_chip, y_chip = lax.rem(gy, RING), 2 * (gy // RING) + gx // RING
    early = jnp.clip(EARLY - x_chip - y_chip - 2 * lax.rem(gx, RING), 0, quads - 3)

    @pl.loop(1, 1 + early)
    def _(quad):
        parameters(quad)
        turn_rows(quad + 1)

    pl.semaphore_wait(barrier, len(around))

    def remote(index, source, target, device):
        copy = pltpu.make_async_remote_copy(
            src_ref=source, dst_ref=target,
            send_sem=send_sem.at[index], recv_sem=recv_sem.at[index],
            device_id=device, device_id_type=MESH,
        )
        copy.start()
        return copy

    copies = [
        remote(4, send_corners.at[0], recv_corners.at[0], (core, xp, yp)),
        remote(5, send_corners.at[1], recv_corners.at[1], (core, xp, yn)),
        remote(6, send_corners.at[2], recv_corners.at[2], (core, xn, yp)),
        remote(7, send_corners.at[3], recv_corners.at[3], (core, xn, yn)),
        remote(0, send_rows.at[0, pl.ds(0, sent)], recv_rows.at[0, pl.ds(0, sent)], (core, xp, gy)),
        remote(1, send_rows.at[1, pl.ds(0, sent)], recv_rows.at[1, pl.ds(0, sent)], (core, xn, gy)),
        remote(2, send_cols.at[0], recv_cols.at[0], (core, gx, yp)),
        remote(3, send_cols.at[1], recv_cols.at[1], (core, gx, yn)),
    ]

    @pl.loop(1 + early, quads - 2)
    def _(quad):
        parameters(quad)
        turn_rows(quad + 1)

    parameters(quads - 2)

    for copy in copies:
        copy.wait_recv()

    for side, quad in ((1, 0), (0, quads - 1)):
        for k in range(ROWS):
            outer = k == (near if side == 0 else 0)
            if outer:
                x = recv_rows[side, pl.ds(fields * near, 2 * SUBLANES), :]
                x = jnp.concatenate([x, jnp.zeros((kpad - 2 * SUBLANES, LANES), F32)], axis=0)
            else:
                x = recv_rows[side, pl.ds(k - side, kpad, stride=near), :]
            lnat[quad % 2, pl.ds(k * ring, LANES), :] = turned(x)
        parameters(quad)

    for t in range(2 * tiles):
        cols_t[pl.ds(t * LANES, LANES), :] = turned(recv_cols[t // tiles, t % tiles])
    corners = [recv_corners[k] for k in range(4)]
    unpacked = []
    for m in range(groups):
        x = jnp.zeros((SUBLANES, LANES), F32)
        for k in range(4):
            x = jnp.where(by_block == k, pltpu.roll(corners[k], block * (k - m) % LANES, 1), x)
        unpacked.append(x)
    cols_t[pl.ds(2 * tiles * LANES, LANES), :] = turned(jnp.concatenate(unpacked, axis=0))

    def column_halo(row, right, left_side):
        halo_l[pl.ds(row * SUBLANES, HALO), :] = cols_t[pl.ds(right, HALO), :]
        halo_l[pl.ds(row * SUBLANES + HALO, HALO), :] = cols_t[pl.ds(left_side, HALO), :]

    for row in range(rows):
        t, g = divmod(row, per_tile)
        column_halo(
            row + HALO,
            t * LANES + HALO * ((g + 1) % per_tile),
            (tiles + t) * LANES + HALO * g,
        )
    corner = 2 * tiles * LANES
    for r in range(HALO):
        column_halo(rows + HALO + r, corner + HALO * r, corner + block + HALO * r)
        column_halo(r, corner + 2 * block + HALO * r, corner + 3 * block + HALO * r)
    edge = (chunk - SUBLANES) * SUBLANES + SUBLANES - 1
    for group in range(5):
        found = nn(halo_l[...].astype(BF16), rhs[group])
        for half, target in enumerate(targets(group)):
            for row in range(ext):
                piece = found[row * SUBLANES : (row + 1) * SUBLANES, half * LANES : (half + 1) * LANES]
                target(row)[pl.ds(edge, SUBLANES, stride=SUBLANES), :] = piece

    tile = [pl.ds(SUBLANES * j, SUBLANES) for j in range(chunk)]

    def advance(step, h, first, number):
        cf = cfs[h].at[pl.ds(first, number)]
        u = us[h].at[pl.ds(first, number + 1)]
        cells = [kept.at[h]] + [u.at[k] for k in range(number + 1)]

        def column(j):
            return [ref[tile[j], :] for ref in cells]

        column_now = column(0)
        last = [ref[tile[chunk - 1], :] for ref in cells[1:-1]]
        wrap = [column_now[k + 1] - pltpu.roll(last[k], 1, 0) for k in range(number)]
        south = wrap
        for j in range(chunk):
            if j + 1 < chunk:
                column_next = column(j + 1)
                north = [column_next[k + 1] - column_now[k + 1] for k in range(number)]
            else:
                column_next = None
                north = [pltpu.roll(x, SUBLANES - 1, 0) for x in wrap]
            east = [column_now[k + 1] - column_now[k] for k in range(number + 1)]
            for k in range(number):
                c = [cf[k, m, tile[j], :] for m in range(4)]
                new = column_now[k + 1] + (
                    (c[0] * east[k + 1] - c[1] * east[k]) + (c[2] * north[k] - c[3] * south[k])
                )
                if step < 4:
                    u[k, tile[j], :] = new
                    continue
                one = node_w[:, h * LANES : (h + 1) * LANES] * new
                two = one * new
                if h == 0:
                    part[k, 0, tile[j], :] = one
                    part[k, 1, tile[j], :] = two
                else:
                    both[k, 0, tile[j], :] = one + part[k, 0, tile[j], :]
                    both[k, 1, tile[j], :] = two + part[k, 1, tile[j], :]
            kept[h, tile[j], :] = column_now[number]
            column_now, south = column_next, north

    def gather_sums(first):
        masks = [(lane == first + k + m * rows, k, m) for k in range(ROWS) for m in range(2)]
        for j in range(chunk):
            old = acc[tile[j], :]
            for mask, k, m in masks:
                old = jnp.where(mask, jnp.sum(both[k, m, tile[j], :], axis=1, keepdims=True), old)
            acc[tile[j], :] = old

    for step in range(1, 5):
        start, needed = step, ext - 2 * step
        for h in range(2):
            kept[h] = us[h][max(start - 1, 0)]
        if step == 4:
            both[...] = jnp.zeros_like(both)

        @pl.loop(0, needed // ROWS)
        def _(turn):
            first = start + ROWS * turn
            if step == 4:
                gather_sums(first - HALO - ROWS)
            for h in range(2):
                advance(step, h, first, ROWS)

        if needed % ROWS:
            for h in range(2):
                advance(step, h, start + needed // ROWS * ROWS, needed % ROWS)

    gather_sums(rows - ROWS)

    for j in range(chunk):
        nat[pl.ds(j, SUBLANES, stride=chunk), :] = acc[tile[j], :]
    mine[...] = jnp.transpose(nat[0:LANES, :])
    swap = remote(8, mine, theirs, (1 - core, gx, gy))
    for copy in copies:
        copy.wait_send()
    swap.wait()
    moments_ref[...] = (mine[...] + theirs[...]) / weight_total


def on_device(mesh, field_modes, node_points, quad_weight, group_of):
    rows, cols = field_modes.shape[2:]
    count, dims = node_points.shape
    modes = dims + 1
    ext = rows + 2 * HALO
    ring = cols + 2 * HALO
    kpad = 40
    tiles = rows * HALO // LANES
    vmem = pl.BlockSpec(memory_space=pltpu.VMEM)
    moments = pl.pallas_call(
        functools.partial(kernel, mesh.shape["gx"], mesh.shape["gy"], rows, dims),
        out_shape=pltpu.VMEM((2 * rows, cols), F32),
        in_specs=[pl.BlockSpec(memory_space=pl.ANY)] * 4,
        out_specs=vmem,
        scratch_shapes=[
            pltpu.VMEM((kpad * (rows + SUBLANES), LANES), F32),
            pltpu.VMEM((2, kpad * (HALO - 1) + SUBLANES, LANES), F32),
            pltpu.VMEM((2, kpad * (HALO - 1) + SUBLANES, LANES), F32),
            pltpu.VMEM((2, tiles, kpad, LANES), F32),
            pltpu.VMEM((2, tiles, kpad, LANES), F32),
            pltpu.VMEM((4, SUBLANES, LANES), F32),
            pltpu.VMEM((4, SUBLANES, LANES), F32),
            pltpu.VMEM((2, ROWS * ring, LANES), F32),
            pltpu.VMEM((ROWS * ring, LANES), BF16),
            pltpu.VMEM(((2 * tiles + 1) * LANES, LANES), F32),
            pltpu.VMEM((ext * SUBLANES, LANES), F32),
            pltpu.VMEM((5, LANES, 2 * LANES), F32),
            pltpu.VMEM((5, LANES, 2 * LANES), BF16),
            pltpu.VMEM((SUBLANES, SLOTS), F32),
            pltpu.VMEM((2 * SUBLANES, SLOTS), F32),
            pltpu.VMEM((ext, 4, ring, LANES), F32),
            pltpu.VMEM((ext, 4, ring, LANES), F32),
            pltpu.VMEM((ext + 1, ring, LANES), F32),
            pltpu.VMEM((ext + 1, ring, LANES), F32),
            pltpu.VMEM((2, ring, LANES), F32),
            pltpu.VMEM((ROWS, 2, ring, LANES), F32),
            pltpu.VMEM((ROWS, 2, ring, LANES), F32),
            pltpu.VMEM((ring, LANES), F32),
            pltpu.VMEM((ring, LANES), F32),
            pltpu.VMEM((2 * rows, LANES), F32),
            pltpu.VMEM((2 * rows, LANES), F32),
            pltpu.VMEM((dims, count), F32),
            pltpu.VMEM((count,), F32),
            pltpu.VMEM((count,), jnp.int32),
            pltpu.SemaphoreType.DMA((4,)),
            pltpu.SemaphoreType.DMA((9,)),
            pltpu.SemaphoreType.DMA((9,)),
        ],
        compiler_params=pltpu.CompilerParams(
            collective_id=0, has_side_effects=True, vmem_limit_bytes=62 * 1024 * 1024
        ),
    )(
        field_modes.reshape(4 * modes * rows, cols),
        node_points.T,
        quad_weight,
        group_of,
    )
    mean_field = moments[:rows]
    return mean_field, moments[rows:] - mean_field * mean_field


def solution(mesh):
    return jax.shard_map(
        functools.partial(on_device, mesh),
        mesh=mesh,
        in_specs=(P(None, None, "gx", "gy"), P(), P(), P()),
        out_specs=(P("gx", "gy"), P("gx", "gy")),
        check_vma=False,
    )
```

```python
import functools

import jax
import jax.numpy as jnp
from jax import lax
from jax.experimental import pallas as pl
from jax.experimental.pallas import tpu as pltpu
from jax.sharding import PartitionSpec as P

TIME_STEP = 0.15
HALO = 4
LANES = 128
SUBLANES = 8
SLOTS = 256
ROWS = 4
EARLY = 12
RING = 4
MESH = pl.DeviceIdType.MESH
F32 = jnp.float32
BF16 = jnp.bfloat16


def nn(a, b):
    return lax.dot_general(a, b, (((1,), (0,)), ((), ())), preferred_element_type=F32)


def nt(a, b):
    return lax.dot_general(a, b, (((1,), (1,)), ((), ())), preferred_element_type=F32)


def split2(x):
    hi = x.astype(BF16).astype(F32)
    return hi, x - hi


def split3(x):
    hi = x.astype(BF16).astype(F32)
    rest = x - hi
    mid = rest.astype(BF16).astype(F32)
    return hi, mid, rest - mid


def kernel(
    gx_size, gy_size, rows, dims,
    field_hbm, points_hbm, weight_hbm, group_hbm,
    moments_ref,
    fv, send_rows, recv_rows, send_cols, recv_cols, send_corners, recv_corners,
    lnat, left, cols_t, halo_l, rhs_f, rhs, node_w, csc,
    cf0, cf1, ua, ub, kept, part, both, acc, nat, mine, theirs,
    points_ref, weight_ref, group_ref,
    load_sem, send_sem, recv_sem,
):
    ext = rows + 2 * HALO
    quads = ext // ROWS
    modes = dims + 1
    fields = 4 * modes
    ring = LANES + 2 * HALO
    chunk = ring // SUBLANES
    kpad = 40
    groups = kpad // SUBLANES
    core = lax.axis_index("nodes")
    gx = lax.axis_index("gx")
    gy = lax.axis_index("gy")
    xn, xp = lax.rem(gx + 1, gx_size), lax.rem(gx + gx_size - 1, gx_size)
    yn, yp = lax.rem(gy + 1, gy_size), lax.rem(gy + gy_size - 1, gy_size)
    around = [
        (core, xp, gy), (core, xn, gy), (core, gx, yp), (core, gx, yn),
        (core, xp, yp), (core, xp, yn), (core, xn, yp), (core, xn, yn),
        (1 - core, gx, gy),
    ]

    barrier = pltpu.get_barrier_semaphore()
    for device in around:
        pl.semaphore_signal(barrier, inc=1, device_id=device, device_id_type=MESH)

    apart = fv.shape[0] // kpad

    @pl.loop(0, fields)
    def _(k):
        pltpu.make_async_copy(
            field_hbm.at[pl.ds(k * rows, rows)], fv.at[pl.ds(k * apart, rows)], load_sem.at[0]
        ).start()

    small = [
        pltpu.make_async_copy(source, target, load_sem.at[1 + i])
        for i, (source, target) in enumerate(
            [(points_hbm, points_ref), (weight_hbm, weight_ref), (group_hbm, group_ref)]
        )
    ]
    for copy in small:
        copy.start()
    fv[pl.ds(fields * apart, (kpad - fields) * apart), :] = jnp.zeros(((kpad - fields) * apart, LANES), F32)

    for copy in small:
        copy.wait()
    count = group_ref.shape[0]
    included = (group_ref[...].reshape(1, count) < 2).astype(F32)
    weights = weight_ref[...].reshape(1, count)
    weight_total = jnp.sum(weights * included, axis=1, keepdims=True)
    row8 = lax.broadcasted_iota(jnp.int32, (SUBLANES, LANES), 0)
    blocks = count // LANES
    pieces = [included[:, b * LANES : (b + 1) * LANES] for b in range(blocks)]
    stacked = jnp.zeros((SUBLANES, LANES), F32)
    for b in range(blocks):
        stacked = jnp.where(row8 == b, jnp.broadcast_to(pieces[b], (SUBLANES, LANES)), stacked)
    before = lax.broadcasted_iota(jnp.int32, (LANES, LANES), 0) <= lax.broadcasted_iota(jnp.int32, (LANES, LANES), 1)
    within = nn(stacked.astype(BF16), before.astype(F32).astype(BF16))
    totals = jnp.sum(stacked, axis=1, keepdims=True)
    slot = (lax.broadcasted_iota(jnp.int32, (SLOTS, LANES), 0) + (core * SLOTS + 1)).astype(F32)
    offset = jnp.zeros((1, 1), F32)
    chosen = []
    for b in range(blocks):
        order = within[b : b + 1] + offset
        offset = offset + totals[b : b + 1]
        order = jnp.where(pieces[b] > 0, order, 0.0)
        chosen.append(jnp.where(slot == jnp.broadcast_to(order, (SLOTS, LANES)), 1.0, 0.0).astype(BF16))
    select = jnp.concatenate(chosen, axis=1)
    w_hi, w_mid, w_lo = split3(weights)
    w_rows = lax.broadcasted_iota(jnp.int32, (SUBLANES, count), 0)
    w_stack = jnp.where(w_rows == 0, w_hi, jnp.where(w_rows == 1, w_mid, jnp.where(w_rows == 2, w_lo, 0.0)))
    found = nt(jnp.concatenate([*split3(points_ref[...]), w_stack], axis=0).astype(BF16), select)
    coords = found[0:dims] + found[dims : 2 * dims] + found[2 * dims : 3 * dims]
    held = found[3 * dims : 3 * dims + 1] + found[3 * dims + 1 : 3 * dims + 2] + found[3 * dims + 2 : 3 * dims + 3]
    node_w[...] = jnp.broadcast_to(held, (SUBLANES, SLOTS))

    csc[0:1, :] = jnp.ones((1, SLOTS), F32)
    csc[1 : 1 + dims, :] = coords
    coefficient = csc[...][0:modes]
    rhs_f[...] = jnp.zeros_like(rhs_f)

    def place(group, half, h, field, scale):
        hi, lo = split2(coefficient[:, h * LANES : (h + 1) * LANES] * scale)
        at = field * modes
        lanes = pl.ds(half * LANES, LANES)
        rhs_f[group, pl.ds(at, modes), lanes] = hi
        rhs_f[group, pl.ds(kpad + at, modes), lanes] = lo
        rhs_f[group, pl.ds(2 * kpad + at, modes), lanes] = hi

    for h in range(2):
        for k in range(4):
            place(2 * h + k // 2, k % 2, h, 3, TIME_STEP)
            place(2 * h + k // 2, k % 2, h, 1 + k // 2, (-0.5, 0.5)[k % 2] * TIME_STEP)
        place(4, h, h, 0, 1.0)
    rhs[...] = rhs_f[...].astype(BF16)

    rest = jnp.zeros((SUBLANES, LANES), F32)

    def turned(x):
        hi, lo = split2(x)
        stack = jnp.concatenate([hi, hi, lo, rest], axis=0).astype(BF16)
        return jnp.transpose(stack).astype(F32)

    def turn_rows(quad):
        for k in range(ROWS):
            x = fv[pl.ds(ROWS * quad - HALO + k, kpad, stride=apart), :]
            lnat[lax.rem(quad, 2), pl.ds(k * ring, LANES), :] = turned(x)

    cfs, us = (cf0, cf1), (ua, ub)

    def targets(group):
        if group == 4:
            return [lambda row: us[0].at[row], lambda row: us[1].at[row]]
        return [
            lambda row: cfs[group // 2].at[row, 2 * (group % 2)],
            lambda row: cfs[group // 2].at[row, 2 * (group % 2) + 1],
        ]

    def parameters(quad):
        slot = lax.rem(quad, 2)
        cells = []
        for k in range(ROWS):
            cells += [lnat[slot, pl.ds(k * ring + j, SUBLANES, stride=chunk), :] for j in range(chunk)]
        left[...] = jnp.concatenate(cells, axis=0).astype(BF16)
        for group in range(5):
            found = nn(left[...], rhs[group])
            for half, target in enumerate(targets(group)):
                for k in range(ROWS):
                    piece = found[k * ring : (k + 1) * ring, half * LANES : (half + 1) * LANES]
                    target(ROWS * quad + k)[...] = piece

    near = HALO - 1
    sent = kpad * near
    for side in range(2):
        recv_rows[side, pl.ds(sent, SUBLANES), :] = jnp.zeros((SUBLANES, LANES), F32)
    acc[...] = jnp.zeros_like(acc)
    pltpu.make_async_copy(field_hbm, fv.at[pl.ds(0, fields * rows)], load_sem.at[0]).wait()

    lane = lax.broadcasted_iota(jnp.int32, (SUBLANES, LANES), 1)
    by_halo = lane // HALO
    block = HALO * HALO
    by_block = lane // block
    per_tile = LANES // HALO
    tiles = rows // per_tile

    for side in range(2):
        for r in range(near):
            row = r if side == 0 else rows - near + r
            send_rows[side, pl.ds(r, kpad, stride=near), :] = fv[pl.ds(row, kpad, stride=apart), :]
        row = near if side == 0 else rows - HALO
        send_rows[side, pl.ds(fields * near, modes), :] = fv[pl.ds(row, modes, stride=apart), :]
    for t in range(tiles):
        low = [jnp.zeros((SUBLANES, LANES), F32)] * groups
        high = [jnp.zeros((SUBLANES, LANES), F32)] * groups
        for g in range(per_tile):
            at_high = by_halo == g
            at_low = by_halo == (g + 1) % per_tile
            for m in range(groups):
                x = fv[pl.ds(m * SUBLANES * apart + t * per_tile + g, SUBLANES, stride=apart), :]
                x = pltpu.roll(x, (HALO * (g + 1)) % LANES, 1)
                high[m] = jnp.where(at_high, x, high[m])
                low[m] = jnp.where(at_low, x, low[m])
        for side, values in enumerate((low, high)):
            for m in range(groups):
                send_cols[side, t, m * SUBLANES : (m + 1) * SUBLANES, :] = values[m]
            for end in range(2):
                if t != (0, tiles - 1)[end]:
                    continue
                at = HALO * (1 - side) + (0, LANES - block)[end]
                packed = jnp.zeros((SUBLANES, LANES), F32)
                for m in range(groups):
                    packed = jnp.where(by_block == m, pltpu.roll(values[m], (block * m - at) % LANES, 1), packed)
                send_corners[2 * end + side] = packed

    turn_rows(1)

    x_chip, y_chip = lax.rem(gy, RING), 2 * (gy // RING) + gx // RING
    early = jnp.clip(EARLY - x_chip - y_chip - 2 * lax.rem(gx, RING), 0, quads - 3)

    @pl.loop(1, 1 + early)
    def _(quad):
        parameters(quad)
        turn_rows(quad + 1)

    pl.semaphore_wait(barrier, len(around))

    def remote(index, source, target, device):
        copy = pltpu.make_async_remote_copy(
            src_ref=source, dst_ref=target,
            send_sem=send_sem.at[index], recv_sem=recv_sem.at[index],
            device_id=device, device_id_type=MESH,
        )
        copy.start()
        return copy

    copies = [
        remote(4, send_corners.at[0], recv_corners.at[0], (core, xp, yp)),
        remote(5, send_corners.at[1], recv_corners.at[1], (core, xp, yn)),
        remote(6, send_corners.at[2], recv_corners.at[2], (core, xn, yp)),
        remote(7, send_corners.at[3], recv_corners.at[3], (core, xn, yn)),
        remote(0, send_rows.at[0, pl.ds(0, sent)], recv_rows.at[0, pl.ds(0, sent)], (core, xp, gy)),
        remote(1, send_rows.at[1, pl.ds(0, sent)], recv_rows.at[1, pl.ds(0, sent)], (core, xn, gy)),
        remote(2, send_cols.at[0], recv_cols.at[0], (core, gx, yp)),
        remote(3, send_cols.at[1], recv_cols.at[1], (core, gx, yn)),
    ]

    @pl.loop(1 + early, quads - 2)
    def _(quad):
        parameters(quad)
        turn_rows(quad + 1)

    parameters(quads - 2)

    for copy in copies:
        copy.wait_recv()

    for side, quad in ((1, 0), (0, quads - 1)):
        for k in range(ROWS):
            outer = k == (near if side == 0 else 0)
            if outer:
                x = recv_rows[side, pl.ds(fields * near, 2 * SUBLANES), :]
                x = jnp.concatenate([x, jnp.zeros((kpad - 2 * SUBLANES, LANES), F32)], axis=0)
            else:
                x = recv_rows[side, pl.ds(k - side, kpad, stride=near), :]
            lnat[quad % 2, pl.ds(k * ring, LANES), :] = turned(x)
        parameters(quad)

    for t in range(2 * tiles):
        cols_t[pl.ds(t * LANES, LANES), :] = turned(recv_cols[t // tiles, t % tiles])
    corners = [recv_corners[k] for k in range(4)]
    unpacked = []
    for m in range(groups):
        x = jnp.zeros((SUBLANES, LANES), F32)
        for k in range(4):
            x = jnp.where(by_block == k, pltpu.roll(corners[k], block * (k - m) % LANES, 1), x)
        unpacked.append(x)
    cols_t[pl.ds(2 * tiles * LANES, LANES), :] = turned(jnp.concatenate(unpacked, axis=0))

    def column_halo(row, right, left_side):
        halo_l[pl.ds(row * SUBLANES, HALO), :] = cols_t[pl.ds(right, HALO), :]
        halo_l[pl.ds(row * SUBLANES + HALO, HALO), :] = cols_t[pl.ds(left_side, HALO), :]

    for row in range(rows):
        t, g = divmod(row, per_tile)
        column_halo(
            row + HALO,
            t * LANES + HALO * ((g + 1) % per_tile),
            (tiles + t) * LANES + HALO * g,
        )
    corner = 2 * tiles * LANES
    for r in range(HALO):
        column_halo(rows + HALO + r, corner + HALO * r, corner + block + HALO * r)
        column_halo(r, corner + 2 * block + HALO * r, corner + 3 * block + HALO * r)
    edge = (chunk - SUBLANES) * SUBLANES + SUBLANES - 1
    for group in range(5):
        found = nn(halo_l[...].astype(BF16), rhs[group])
        for half, target in enumerate(targets(group)):
            for row in range(ext):
                piece = found[row * SUBLANES : (row + 1) * SUBLANES, half * LANES : (half + 1) * LANES]
                target(row)[pl.ds(edge, SUBLANES, stride=SUBLANES), :] = piece

    tile = [pl.ds(SUBLANES * j, SUBLANES) for j in range(chunk)]

    def advance(step, h, first, number):
        cf = cfs[h].at[pl.ds(first, number)]
        u = us[h].at[pl.ds(first, number + 1)]
        cells = [kept.at[h]] + [u.at[k] for k in range(number + 1)]

        def column(j):
            return [ref[tile[j], :] for ref in cells]

        column_now = column(0)
        last = [ref[tile[chunk - 1], :] for ref in cells[1:-1]]
        wrap = [column_now[k + 1] - pltpu.roll(last[k], 1, 0) for k in range(number)]
        south = wrap
        for j in range(chunk):
            if j + 1 < chunk:
                column_next = column(j + 1)
                north = [column_next[k + 1] - column_now[k + 1] for k in range(number)]
            else:
                column_next = None
                north = [pltpu.roll(x, SUBLANES - 1, 0) for x in wrap]
            east = [column_now[k + 1] - column_now[k] for k in range(number + 1)]
            for k in range(number):
                c = [cf[k, m, tile[j], :] for m in range(4)]
                new = column_now[k + 1] + (
                    (c[0] * east[k + 1] - c[1] * east[k]) + (c[2] * north[k] - c[3] * south[k])
                )
                if step < 4:
                    u[k, tile[j], :] = new
                    continue
                one = node_w[:, h * LANES : (h + 1) * LANES] * new
                two = one * new
                if h == 0:
                    part[k, 0, tile[j], :] = one
                    part[k, 1, tile[j], :] = two
                else:
                    both[k, 0, tile[j], :] = one + part[k, 0, tile[j], :]
                    both[k, 1, tile[j], :] = two + part[k, 1, tile[j], :]
            kept[h, tile[j], :] = column_now[number]
            column_now, south = column_next, north

    def gather_sums(first):
        masks = [(lane == first + k + m * rows, k, m) for k in range(ROWS) for m in range(2)]
        for j in range(chunk):
            old = acc[tile[j], :]
            for mask, k, m in masks:
                old = jnp.where(mask, jnp.sum(both[k, m, tile[j], :], axis=1, keepdims=True), old)
            acc[tile[j], :] = old

    for step in range(1, 5):
        start, needed = step, ext - 2 * step
        for h in range(2):
            kept[h] = us[h][max(start - 1, 0)]
        if step == 4:
            both[...] = jnp.zeros_like(both)

        @pl.loop(0, needed // ROWS)
        def _(turn):
            first = start + ROWS * turn
            if step == 4:
                gather_sums(first - HALO - ROWS)
            for h in range(2):
                advance(step, h, first, ROWS)

        if needed % ROWS:
            for h in range(2):
                advance(step, h, start + needed // ROWS * ROWS, needed % ROWS)

    gather_sums(rows - ROWS)

    for j in range(chunk):
        nat[pl.ds(j, SUBLANES, stride=chunk), :] = acc[tile[j], :]
    mine[...] = jnp.transpose(nat[0:LANES, :])
    swap = remote(8, mine, theirs, (1 - core, gx, gy))
    for copy in copies:
        copy.wait_send()
    swap.wait()
    moments_ref[...] = (mine[...] + theirs[...]) / weight_total


def on_device(mesh, field_modes, node_points, quad_weight, group_of):
    rows, cols = field_modes.shape[2:]
    count, dims = node_points.shape
    modes = dims + 1
    ext = rows + 2 * HALO
    ring = cols + 2 * HALO
    kpad = 40
    tiles = rows * HALO // LANES
    vmem = pl.BlockSpec(memory_space=pltpu.VMEM)
    moments = pl.pallas_call(
        functools.partial(kernel, mesh.shape["gx"], mesh.shape["gy"], rows, dims),
        out_shape=pltpu.VMEM((2 * rows, cols), F32),
        in_specs=[pl.BlockSpec(memory_space=pl.ANY)] * 4,
        out_specs=vmem,
        scratch_shapes=[
            pltpu.VMEM((kpad * (rows + SUBLANES), LANES), F32),
            pltpu.VMEM((2, kpad * (HALO - 1) + SUBLANES, LANES), F32),
            pltpu.VMEM((2, kpad * (HALO - 1) + SUBLANES, LANES), F32),
            pltpu.VMEM((2, tiles, kpad, LANES), F32),
            pltpu.VMEM((2, tiles, kpad, LANES), F32),
            pltpu.VMEM((4, SUBLANES, LANES), F32),
            pltpu.VMEM((4, SUBLANES, LANES), F32),
            pltpu.VMEM((2, ROWS * ring, LANES), F32),
            pltpu.VMEM((ROWS * ring, LANES), BF16),
            pltpu.VMEM(((2 * tiles + 1) * LANES, LANES), F32),
            pltpu.VMEM((ext * SUBLANES, LANES), F32),
            pltpu.VMEM((5, LANES, 2 * LANES), F32),
            pltpu.VMEM((5, LANES, 2 * LANES), BF16),
            pltpu.VMEM((SUBLANES, SLOTS), F32),
            pltpu.VMEM((2 * SUBLANES, SLOTS), F32),
            pltpu.VMEM((ext, 4, ring, LANES), F32),
            pltpu.VMEM((ext, 4, ring, LANES), F32),
            pltpu.VMEM((ext + 1, ring, LANES), F32),
            pltpu.VMEM((ext + 1, ring, LANES), F32),
            pltpu.VMEM((2, ring, LANES), F32),
            pltpu.VMEM((ROWS, 2, ring, LANES), F32),
            pltpu.VMEM((ROWS, 2, ring, LANES), F32),
            pltpu.VMEM((ring, LANES), F32),
            pltpu.VMEM((ring, LANES), F32),
            pltpu.VMEM((2 * rows, LANES), F32),
            pltpu.VMEM((2 * rows, LANES), F32),
            pltpu.VMEM((dims, count), F32),
            pltpu.VMEM((count,), F32),
            pltpu.VMEM((count,), jnp.int32),
            pltpu.SemaphoreType.DMA((4,)),
            pltpu.SemaphoreType.DMA((9,)),
            pltpu.SemaphoreType.DMA((9,)),
        ],
        compiler_params=pltpu.CompilerParams(
            collective_id=0, has_side_effects=True, vmem_limit_bytes=62 * 1024 * 1024
        ),
    )(
        field_modes.reshape(4 * modes * rows, cols),
        node_points.T,
        quad_weight,
        group_of,
    )
    mean_field = moments[:rows]
    return mean_field, moments[rows:] - mean_field * mean_field


def solution(mesh):
    return jax.shard_map(
        functools.partial(on_device, mesh),
        mesh=mesh,
        in_specs=(P(None, None, "gx", "gy"), P(), P(), P()),
        out_specs=(P("gx", "gy"), P("gx", "gy")),
        check_vma=False,
    )
```
